128 devices in a mesh: seq: 64 (over z_hi, x, y, core), head: 2 (over z_lo).
Axes of the slice: x: 4, y: 4, z: 4 (z_hi: 2, z_lo: 2; z = z_hi * 2 + z_lo), core: 2. Of those that a mesh axis runs over, the one named last changes fastest.
Arguments:
- tokens: bfloat16 [32768, 3584], P('seq', 'head'), may hold values from -6 to 6
- pre_gain: float32 [3584], replicated, may hold values from 0.5 to 1.5
- query_weight: bfloat16 [3584, 2048], P(None, 'head'), may hold values from -0.375 to 0.375
- key_weight: bfloat16 [3584, 1024], P(None, 'head'), may hold values from -0.375 to 0.375
- value_weight: bfloat16 [3584, 1024], P(None, 'head'), may hold values from -0.09375 to 0.09375
- out_weight: bfloat16 [2048, 3584], P('head'), may hold values from -0.5 to 0.5
- post_gain: float32 [3584], P('head'), may hold values from 0.5 to 1.5
Outputs:
- layer_out: bfloat16 [32768, 3584], P('seq', 'head')
The draws below stay inside these ranges and needn't reach their ends.
All inputs are finite; a program needn't handle non-finite values.
Results may differ from the reference program's by a relative error of at most 0.013.
The reference program's roundings to bfloat16 on the way count: a program that leaves them out, or rounds other values in their place, can miss the bound.
Values may be sent and summed in bfloat16 or wider, within the bound.
A program may use at most 192 MiB of HBM per device.

```python
import jax
import jax.numpy as jnp
from jax import lax

D = 3584
QH = 8
KVH = 4
HD = 256
WINDOW = 4096
TOK_DEV = 512
TOKENS = 32768


def draw_out_weight(key, part):
    key_entries = jax.random.fold_in(key, 11)
    key_columns = jax.random.fold_in(key, 12)
    fan_in = QH * HD
    ramp = 3.0 ** (jnp.arange(D, dtype=jnp.float32) / D)
    column_scale = jnp.exp(jax.random.uniform(key_columns, (D,), jnp.float32) * jnp.log(10.0)) * ramp / 6.0
    entries = jax.random.truncated_normal(key_entries, -4.0, 4.0, (fan_in, D), jnp.float32)
    matrix = entries * column_scale[None, :] * (fan_in * 1.0) ** (-0.5)
    return jnp.clip(matrix, -0.5, 0.5).astype(jnp.bfloat16)


def block_scale(stream_key, shape, split, smallest, high):
    level = 1.0
    for dim, shards_of in split:
        steps = jax.random.uniform(jax.random.fold_in(jax.random.fold_in(stream_key, 6), dim), (shards_of,), jnp.float32, smallest / len(split), high / len(split))
        level = level * jnp.repeat(jnp.exp(steps), shape[dim] // shards_of).reshape((-1,) + (1,) * (len(shape) - 1 - dim))
    return level


def scatter_about(rng, shape, width, limit, pieces=(), held_as=jnp.bfloat16):
    drawn = width * jax.random.normal(rng, shape, jnp.float32)
    if pieces:
        drawn = drawn * block_scale(rng, shape, pieces, -0.22, 0.18)
    return jnp.clip(drawn, -limit, limit).astype(held_as)


def setup_inputs(seed: int = 0) -> dict:
    streams_of = jax.random.split(jax.random.key(seed), 8)
    return {
        "tokens": scatter_about(streams_of[0], (TOKENS, D), 1.0, 6.0, ((0, 64), (1, 2))),
        "pre_gain": jnp.clip(1.0 + 0.1 * jax.random.normal(streams_of[1], (D,), jnp.float32), 0.5, 1.5),
        "query_weight": scatter_about(streams_of[2], (D, QH * HD), (D // 16) ** -0.5, 0.375, ((1, 2),)),
        "key_weight": scatter_about(streams_of[3], (D, KVH * HD), (D // 16) ** -0.5, 0.375, ((1, 2),)),
        "value_weight": scatter_about(streams_of[4], (D, KVH * HD), D ** -0.5, 0.09375, ((1, 2),)),
        "out_weight": draw_out_weight(jax.random.fold_in(streams_of[7], 71), 0),
        "post_gain": jnp.clip(1.0 + 0.1 * jax.random.normal(streams_of[6], (D,), jnp.float32), 0.5, 1.5),
    }


softcap_limit = 50.0
rope_base = 10000.0
norm_epsilon = 1e-06

def rms_scale(values):
    return lax.rsqrt(lax.optimization_barrier(jnp.sum(values * values, axis=-1, keepdims=True)) / values.shape[-1] + norm_epsilon)

def rotate(values, positions):
    midpoint = values.shape[-1] // 2
    frequency = jnp.exp(-jnp.log(rope_base) * (2.0 * jnp.arange(midpoint, dtype=jnp.float32) / values.shape[-1]))
    angles = positions.astype(jnp.float32)[:, None] * frequency[None, :]
    cosine = jnp.cos(angles)[:, None, :]
    sine_part = jnp.sin(angles)[:, None, :]
    leading = values[..., :midpoint]
    trailing = values[..., midpoint:]
    return jnp.concatenate([leading * cosine - trailing * sine_part, trailing * cosine + leading * sine_part], axis=-1)

def reference(tokens, pre_gain, query_weight, key_weight, value_weight, out_weight, post_gain):
    widened = tokens.astype(jnp.float32)
    normed = (widened * rms_scale(widened) * pre_gain).astype(jnp.bfloat16)
    positions = jnp.arange(TOKENS, dtype=jnp.int32)
    queries = rotate(jnp.dot(normed, query_weight, preferred_element_type=jnp.float32).reshape(TOKENS, QH, HD), positions).astype(jnp.bfloat16)
    keys_all = rotate(jnp.dot(normed, key_weight, preferred_element_type=jnp.float32).reshape(TOKENS, KVH, HD), positions).astype(jnp.bfloat16)
    values_all = jnp.dot(normed, value_weight, preferred_element_type=jnp.float32).reshape(TOKENS, KVH, HD).astype(jnp.bfloat16)
    queries = lax.optimization_barrier(queries).astype(jnp.float32)
    keys_all = lax.optimization_barrier(keys_all).astype(jnp.float32)
    values_all = lax.optimization_barrier(values_all).astype(jnp.float32)
    group_size = QH // KVH
    padding = jnp.zeros((WINDOW, KVH, HD), jnp.float32)
    keys_padded = jnp.concatenate([padding, keys_all], axis=0)
    values_padded = jnp.concatenate([padding, values_all], axis=0)

    def one_block(block_index):
        first_row = block_index * TOK_DEV
        query_block = lax.dynamic_slice_in_dim(queries, first_row, TOK_DEV, 0).reshape(TOK_DEV, KVH, group_size, HD)
        key_block = lax.dynamic_slice_in_dim(keys_padded, first_row, WINDOW + TOK_DEV, 0)
        value_block = lax.dynamic_slice_in_dim(values_padded, first_row, WINDOW + TOK_DEV, 0)
        query_index = first_row + jnp.arange(TOK_DEV, dtype=jnp.int32)
        key_index = first_row - WINDOW + jnp.arange(WINDOW + TOK_DEV, dtype=jnp.int32)
        scores = jnp.einsum('qkgd,skd->kgqs', query_block, key_block) * HD ** (-0.5)
        capped = softcap_limit * jnp.tanh(scores / softcap_limit)
        offset = query_index[:, None] - key_index[None, :]
        allowed = (offset >= 0) & (offset < WINDOW) & (key_index[None, :] >= 0)
        weights = jnp.where(allowed, jnp.exp(capped), 0.0)
        denominator = lax.optimization_barrier(jnp.sum(weights, axis=-1))
        rounded = lax.optimization_barrier(weights.astype(jnp.bfloat16)).astype(jnp.float32)
        numerator = jnp.einsum('kgqs,skd->qkgd', rounded, value_block)
        attended_block = numerator / jnp.transpose(denominator, (2, 0, 1))[..., None]
        return attended_block.astype(jnp.bfloat16).reshape(TOK_DEV, QH * HD)
    attended = lax.map(one_block, jnp.arange(TOKENS // TOK_DEV, dtype=jnp.int32)).reshape(TOKENS, QH * HD)
    branch = jnp.dot(attended, out_weight, preferred_element_type=jnp.float32)
    return (widened + post_gain * branch * rms_scale(branch)).astype(jnp.bfloat16)
```

```python
import functools
import math

import jax
import jax.numpy as jnp
from jax import lax
from jax.experimental import pallas as pl
from jax.experimental.pallas import tpu as pltpu
from jax.sharding import PartitionSpec as P

D = 3584
HALF = 1792
HD = 256
ROWS = 512
CHUNKS = 4
PART = ROWS // CHUNKS
SLOTS = 9
MESH = pl.DeviceIdType.MESH
F32 = jnp.float32
BF16 = jnp.bfloat16
softcap_limit = 50.0
rope_base = 10000.0
norm_epsilon = 1e-06


def place():
    s = lax.axis_index("seq")
    head = lax.axis_index("head")
    core = lax.rem(s, 2)
    chip = lax.div(s, 2)
    y = lax.rem(chip, 4)
    return s, head, core, chip, y


def rope_tables(row_count):
    positions = lax.axis_index("seq") * row_count + jnp.arange(row_count, dtype=jnp.int32)
    frequency = jnp.exp(-jnp.log(rope_base) * (2.0 * jnp.arange(HD // 2, dtype=F32) / HD))
    angles = positions.astype(F32)[:, None] * frequency[None, :]
    return jnp.cos(angles), jnp.sin(angles)


def slot_rows(slot, chunk):
    return pl.ds(pl.multiple_of((SLOTS - 1 - slot) * ROWS + chunk * PART, PART), PART)


def qkv_kernel(
    tok, gain, wq, wk, wv, cosine, sine, q_out, kv,
    xbuf, xn, wqb, wkb, wvb, load_sem, z_send, z_recv, send, recv, pair_send, pair_recv,
):
    s, head, core, chip, y = place()
    seq_up = s + jnp.where(y < 3, 2, -6)
    seq_down = s + jnp.where(y > 0, -2, 6)
    sibling = s + 1 - 2 * core
    has_next = chip < 28
    has_prev = chip >= 4

    def at_seq(target):
        return (target, head)

    loads = [
        pltpu.make_async_copy(tok, xbuf.at[head], load_sem.at[0]),
        pltpu.make_async_copy(wk, wkb, load_sem.at[1]),
        pltpu.make_async_copy(wv, wvb, load_sem.at[2]),
        pltpu.make_async_copy(wq, wqb, load_sem.at[3]),
    ]
    for load in loads:
        load.start()

    barrier = pltpu.get_barrier_semaphore()
    for target in (at_seq(sibling), (s, 1 - head), at_seq(seq_up), at_seq(seq_down)):
        pl.semaphore_signal(barrier, inc=1, device_id=target, device_id_type=MESH)

    @pl.when(has_next)
    def _():
        pl.semaphore_signal(barrier, inc=1, device_id=at_seq(s + 8), device_id_type=MESH)

    @pl.when(has_prev)
    def _():
        pl.semaphore_signal(barrier, inc=1, device_id=at_seq(s - 8), device_id_type=MESH)

    pl.semaphore_wait(barrier, 4 + has_next.astype(jnp.int32) + has_prev.astype(jnp.int32))

    def token_copy(i):
        rows = pl.ds(pl.multiple_of(i * PART, PART), PART)
        return pltpu.make_async_remote_copy(
            src_ref=tok.at[rows],
            dst_ref=xbuf.at[head, rows],
            send_sem=z_send.at[i],
            recv_sem=z_recv.at[i],
            device_id=(s, 1 - head),
            device_id_type=MESH,
        )

    def token_arrival(i):
        rows = pl.ds(pl.multiple_of(i * PART, PART), PART)
        return pltpu.make_async_remote_copy(
            src_ref=tok.at[rows],
            dst_ref=xbuf.at[1 - head, rows],
            send_sem=z_send.at[i],
            recv_sem=z_recv.at[i],
            device_id=(s, 1 - head),
            device_id_type=MESH,
        )

    def flow(index, i, source, slot, target):
        return pltpu.make_async_remote_copy(
            src_ref=kv.at[slot_rows(source, i)],
            dst_ref=kv.at[slot_rows(slot, i)],
            send_sem=send.at[index, i],
            recv_sem=recv.at[index, i],
            device_id=at_seq(target),
            device_id_type=MESH,
        )

    def far(i):
        return flow(0, i, 0, 8, s + 8)

    def up(i):
        return flow(1, i, jnp.where(y < 3, 0, 8), 2, seq_up)

    def down(i):
        return flow(2, i, jnp.where(y == 0, 0, 8), 6, seq_down)

    def second_up(i):
        return flow(3, i, 2, 4, seq_up)

    def second_down(i):
        return pltpu.make_async_remote_copy(
            src_ref=kv.at[slot_rows(6, i)],
            dst_ref=kv.at[slot_rows(4, i)],
            send_sem=send.at[4, i],
            recv_sem=recv.at[3, i],
            device_id=at_seq(seq_down),
            device_id_type=MESH,
        )

    def to_sibling(i, slot):
        target = slot + 1 - 2 * core
        lane = lax.div(target - 1, 2)
        return pltpu.make_async_remote_copy(
            src_ref=kv.at[slot_rows(slot, i)],
            dst_ref=kv.at[slot_rows(target, i)],
            send_sem=pair_send.at[lane, i],
            recv_sem=pair_recv.at[lane, i],
            device_id=at_seq(sibling),
            device_id_type=MESH,
        )

    def when(condition, action):
        pl.when(condition)(action)

    up_own = y < 3
    up_relay = (y == 3) & has_prev
    down_own = y == 0
    down_relay = (y > 0) & has_prev
    second_up_valid = (y < 3) & (chip >= 1)
    second_down_valid = (y == 1) & has_prev

    for i in range(CHUNKS):
        token_copy(i).start()
    for load in loads:
        load.wait()

    def roped(values, rows):
        cos = cosine[rows]
        sin = sine[rows]
        leading = values[:, : HD // 2]
        trailing = values[:, HD // 2 :]
        return jnp.concatenate([leading * cos - trailing * sin, trailing * cos + leading * sin], axis=1).astype(BF16)

    def own(i):
        token_arrival(i).wait_recv()
        rows = pl.ds(pl.multiple_of(i * PART, PART), PART)
        first = xbuf[0, rows].astype(F32)
        second = xbuf[1, rows].astype(F32)
        squares = jnp.sum(first * first, axis=-1, keepdims=True) + jnp.sum(second * second, axis=-1, keepdims=True)
        scale = lax.rsqrt(squares / D + norm_epsilon)
        xn[:, :HALF] = (first * scale * gain[:, :HALF]).astype(BF16)
        xn[:, HALF:] = (second * scale * gain[:, HALF:]).astype(BF16)

        def key(j, carry):
            columns = pl.ds(pl.multiple_of(j * HD, HD), HD)
            out = jnp.dot(xn[...], wkb[:, columns], preferred_element_type=F32)
            kv[slot_rows(0, i), columns] = roped(out, rows)
            return carry

        def value(j, carry):
            columns = pl.ds(pl.multiple_of(j * HD, HD), HD)
            out = jnp.dot(xn[...], wvb[:, columns], preferred_element_type=F32)
            kv[slot_rows(0, i), pl.ds(pl.multiple_of(2 * HD + j * HD, HD), HD)] = out.astype(BF16)
            return carry

        def query(j, carry):
            columns = pl.ds(pl.multiple_of(j * HD, HD), HD)
            out = jnp.dot(xn[...], wqb[:, columns], preferred_element_type=F32)
            q_out[j, rows] = roped(out, rows)
            return carry

        lax.fori_loop(0, 2, value, 0)
        lax.fori_loop(0, 2, key, 0)
        when(has_next, lambda: far(i).start())
        when(up_own, lambda: up(i).start())
        when(down_own, lambda: down(i).start())
        when(core == 0, lambda: to_sibling(i, 0).start())
        lax.fori_loop(0, 4, query, 0)

    def relay_far(i):
        @pl.when(has_prev)
        def _():
            far(i).wait_recv()
            when(up_relay, lambda: up(i).start())
            when(down_relay, lambda: down(i).start())
            when(core == 1, lambda: to_sibling(i, 8).start())

    def relay_near(i):
        @pl.when(chip >= 1)
        def _():
            up(i).wait_recv()
            when(second_up_valid, lambda: second_up(i).start())
            to_sibling(i, 2).start()

        @pl.when(chip >= 3)
        def _():
            down(i).wait_recv()
            when(second_down_valid, lambda: second_down(i).start())
            to_sibling(i, 6).start()

    def relay_second(i):
        @pl.when(chip >= 2)
        def _():
            second_up(i).wait_recv()
            to_sibling(i, 4).start()

    def step(i, carry):
        @pl.when(i < CHUNKS)
        def _():
            own(i)

        @pl.when((i >= 1) & (i < CHUNKS + 1))
        def _():
            relay_far(i - 1)

        @pl.when((i >= 2) & (i < CHUNKS + 2))
        def _():
            relay_near(i - 2)

        @pl.when(i >= 3)
        def _():
            relay_second(i - 3)

        return carry

    lax.fori_loop(0, CHUNKS + 3, step, 0)

    def drain(i, carry):
        token_copy(i).wait_send()
        when(has_next, lambda: far(i).wait_send())
        when(up_own | up_relay, lambda: up(i).wait_send())
        when(down_own | down_relay, lambda: down(i).wait_send())
        when(second_up_valid, lambda: second_up(i).wait_send())
        when(second_down_valid, lambda: second_down(i).wait_send())
        for slot in (0, 2, 4, 6, 8):
            sends = (slot <= s) & ((core == 0) if slot == 0 else (core == 1) if slot == 8 else (core >= 0))
            when(sends, lambda: to_sibling(i, slot).wait_send())
        for lane in range(4):
            @pl.when(s >= 2 * lane + 1)
            def _():
                pltpu.make_async_remote_copy(
                    src_ref=kv.at[slot_rows(0, i)],
                    dst_ref=kv.at[slot_rows(2 * lane + 1, i)],
                    send_sem=pair_send.at[lane, i],
                    recv_sem=pair_recv.at[lane, i],
                    device_id=at_seq(sibling),
                    device_id_type=MESH,
                ).wait_recv()
        return carry

    lax.fori_loop(0, CHUNKS, drain, 0)


EXP_SCALE = softcap_limit * math.log2(math.e)
SCORE_SCALE = HD ** (-0.5) / softcap_limit
TILE = 256


def attention_kernel(q, kv, out, acc, den):
    s = lax.axis_index("seq")

    def unit(u, carry):
        group = lax.div(u, 2)
        tile = lax.rem(u, 2)
        key_columns = pl.ds(pl.multiple_of(group * HD, HD), HD)
        value_columns = pl.ds(pl.multiple_of(2 * HD + group * HD, HD), HD)
        query = q[pl.ds(2 * group, 2), pl.ds(pl.multiple_of(tile * TILE, TILE), TILE)].reshape(2 * TILE, HD)

        def block(index, count, mask):
            rows = pl.ds(pl.multiple_of(index * TILE, TILE), count * TILE)
            scores = lax.dot_general(
                query, kv[rows, key_columns], (((1,), (1,)), ((), ())), preferred_element_type=F32
            )
            weights = jnp.exp2(EXP_SCALE * jnp.tanh(scores * SCORE_SCALE))
            if mask is not None:
                weights = jnp.where(mask, weights, 0.0)
            partial = weights[:, :128]
            for part in range(1, count * 2):
                partial = partial + weights[:, part * 128 : (part + 1) * 128]
            product = jnp.dot(weights.astype(BF16), kv[rows, value_columns], preferred_element_type=F32)
            return partial, product

        query_row = lax.rem(lax.broadcasted_iota(jnp.int32, (2 * TILE, TILE), 0), TILE)
        key_row = lax.broadcasted_iota(jnp.int32, (2 * TILE, TILE), 1)
        partial, product = block(16 + tile, 1, key_row <= query_row)
        den[...] = partial
        acc[...] = product

        @pl.when(s >= 8)
        def _():
            partial, product = block(tile, 1, key_row > query_row)
            den[...] += partial
            acc[...] += product

        total = jnp.minimum(15, 2 * s + tile)
        groups = lax.div(total, 3)

        def triple(j, carry):
            partial, product = block(13 + tile - 3 * j, 3, None)
            den[...] += partial
            acc[...] += product
            return carry

        def single(j, carry):
            partial, product = block(15 + tile - 3 * groups - j, 1, None)
            den[...] += partial
            acc[...] += product
            return carry

        lax.fori_loop(0, groups, triple, 0)
        lax.fori_loop(0, total - 3 * groups, single, 0)
        denominator = jnp.sum(den[...], axis=-1, keepdims=True)
        attended = (acc[...] / denominator).astype(BF16)
        rows = pl.ds(pl.multiple_of(tile * TILE, TILE), TILE)
        for member in range(2):
            columns = pl.ds(pl.multiple_of((2 * group + member) * HD, HD), HD)
            out[rows, columns] = attended[member * TILE : (member + 1) * TILE]
        return carry

    lax.fori_loop(0, 4, unit, 0)


def in_blocks(shard, dim, length):
    before, after = (shard.shape[:dim], shard.shape[dim + 1 :])
    return jnp.moveaxis(shard.reshape(*before, length, -1, *after), dim, 0)


def local(tokens, pre_gain, query_weight, key_weight, value_weight, out_weight, post_gain):
    cosine, sine = rope_tables(ROWS)
    vmem = pl.BlockSpec(memory_space=pltpu.VMEM)
    hbm = pl.BlockSpec(memory_space=pl.ANY)
    dma = pltpu.SemaphoreType.DMA
    queries, keys_values = pl.pallas_call(
        qkv_kernel,
        out_shape=(
            jax.ShapeDtypeStruct((4, ROWS, HD), BF16),
            jax.ShapeDtypeStruct((SLOTS * ROWS, 4 * HD), BF16),
        ),
        in_specs=[hbm, vmem, hbm, hbm, hbm, vmem, vmem],
        out_specs=(vmem, vmem),
        scratch_shapes=[
            pltpu.VMEM((2, ROWS, HALF), BF16),
            pltpu.VMEM((PART, D), BF16),
            pltpu.VMEM((D, 4 * HD), BF16),
            pltpu.VMEM((D, 2 * HD), BF16),
            pltpu.VMEM((D, 2 * HD), BF16),
            dma((4,)),
            dma((CHUNKS,)),
            dma((CHUNKS,)),
            dma((5, CHUNKS)),
            dma((4, CHUNKS)),
            dma((4, CHUNKS)),
            dma((4, CHUNKS)),
        ],
        compiler_params=pltpu.CompilerParams(
            collective_id=0, has_side_effects=True, vmem_limit_bytes=60 * 1024 * 1024
        ),
        name="qkv",
    )(tokens, pre_gain[None, :], query_weight, key_weight, value_weight, cosine, sine)
    attended = pl.pallas_call(
        attention_kernel,
        out_shape=jax.ShapeDtypeStruct((ROWS, 4 * HD), BF16),
        in_specs=[vmem, vmem],
        out_specs=vmem,
        scratch_shapes=[pltpu.VMEM((2 * TILE, HD), F32), pltpu.VMEM((2 * TILE, 128), F32)],
        compiler_params=pltpu.CompilerParams(vmem_limit_bytes=60 * 1024 * 1024),
        name="attention",
    )(queries, keys_values)
    partial_branch = jnp.dot(attended, out_weight, preferred_element_type=F32)
    blocks = in_blocks(partial_branch.astype(BF16), 1, 2)
    arrived = lax.all_to_all(blocks, "head", split_axis=0, concat_axis=0, tiled=True)
    share = arrived.astype(F32).sum(axis=0)
    squares = lax.all_gather(jnp.sum(share * share, axis=1, keepdims=True), "head").sum(0)
    inverse_rms = lax.rsqrt(squares / D + norm_epsilon)
    return (tokens.astype(F32) + post_gain * share * inverse_rms).astype(BF16)


def solution(mesh):
    placed = (
        P("seq", "head"),
        P(),
        P(None, "head"),
        P(None, "head"),
        P(None, "head"),
        P("head", None),
        P("head"),
    )
    return jax.shard_map(
        local, mesh=mesh, in_specs=placed, out_specs=P("seq", "head"), check_vma=False
    )
```

```python
import math

import jax
import jax.numpy as jnp
from jax import lax
from jax.experimental import pallas as pl
from jax.experimental.pallas import tpu as pltpu
from jax.sharding import PartitionSpec as P

D = 3584
HALF = 1792
HD = 256
ROWS = 512
CHUNKS = 8
PART = ROWS // CHUNKS
SLOTS = 9
TILE = 256
UNITS = 4
MESH = pl.DeviceIdType.MESH
F32 = jnp.float32
BF16 = jnp.bfloat16
softcap_limit = 50.0
rope_base = 10000.0
norm_epsilon = 1e-06
EXP_SCALE = softcap_limit * math.log2(math.e)
SCORE_SCALE = HD ** (-0.5) / softcap_limit


def rope_tables(row_count):
    positions = lax.axis_index("seq") * row_count + jnp.arange(row_count, dtype=jnp.int32)
    frequency = jnp.exp(-jnp.log(rope_base) * (2.0 * jnp.arange(HD // 2, dtype=F32) / HD))
    angles = positions.astype(F32)[:, None] * frequency[None, :]
    return jnp.cos(angles), jnp.sin(angles)


def aligned(start, size, step=None):
    return pl.ds(pl.multiple_of(start, step or size), size)


def slot_rows(slot, chunk):
    return aligned((SLOTS - 1 - slot) * ROWS + chunk * PART, PART)


def when(condition, action):
    pl.when(condition)(action)


def layer_kernel(
    tok, gain, wq, wk, wv, wo, post, cosine, sine, out,
    xbuf, xn, wqb, wkb, wvb, wob, q, kv, acc, den, att, branch, transit, sums, obuf,
    load_sem, z_send, z_recv, send, recv, pair_send, pair_recv,
    transit_send, transit_recv, onward_send, w_send, w_recv, att_send, att_recv, sum_send, sum_recv, out_sem,
):
    s = lax.axis_index("seq")
    head = lax.axis_index("head")
    core = lax.rem(s, 2)
    chip = lax.div(s, 2)
    y = lax.rem(chip, 4)
    x = lax.rem(lax.div(chip, 4), 4)
    z = lax.div(chip, 16)
    other = 1 - head
    seq_up = s + jnp.where(y < 3, 2, -6)
    seq_down = s + jnp.where(y > 0, -2, 6)
    sibling = s + 1 - 2 * core
    has_next = chip < 28
    has_prev = chip >= 4
    crosses = (z == 0) & (x == 3)
    ring_y = [s + 2 * (lax.rem(y + k, 4) - y) for k in (1, 2, 3)]
    ring_x = [s + 8 * (lax.rem(x + k, 4) - x) for k in (1, 2, 3)]

    def at_seq(target):
        return (target, head)

    partner = (s, other)

    def remote(source, target, send_sem, recv_sem, device):
        return pltpu.make_async_remote_copy(
            src_ref=source, dst_ref=target, send_sem=send_sem, recv_sem=recv_sem,
            device_id=device, device_id_type=MESH,
        )

    own_columns = aligned(head * HALF, HALF, 128)
    other_columns = aligned(other * HALF, HALF, 128)
    loads = [
        pltpu.make_async_copy(tok, xbuf.at[head], load_sem.at[0]),
        pltpu.make_async_copy(wv, wvb, load_sem.at[1]),
        pltpu.make_async_copy(wk, wkb, load_sem.at[2]),
        pltpu.make_async_copy(wq, wqb, load_sem.at[3]),
        pltpu.make_async_copy(wo.at[:, own_columns], wob.at[aligned(head * 1024, 1024)], load_sem.at[4]),
    ]
    for load in loads:
        load.start()

    barrier = pltpu.get_barrier_semaphore()

    def greet(device):
        pl.semaphore_signal(barrier, inc=1, device_id=device, device_id_type=MESH)

    greet(partner)
    greet(at_seq(sibling))
    for target in ring_y + ring_x:
        greet(at_seq(target))

    @pl.when(z == 1)
    def _():
        greet(at_seq((12 + y) * 2 + core))

    @pl.when(crosses)
    def _():
        for column in range(4):
            greet(at_seq((16 + 4 * column + y) * 2 + core))

    pl.semaphore_wait(barrier, 8 + z + 4 * crosses.astype(jnp.int32))

    slice_index = (core * 4 + x) * 4 + y
    mine = head * 1024
    theirs = other * 1024

    def weight_slice():
        return remote(
            wo.at[aligned(slice_index * 32, 32), other_columns], wob.at[aligned(mine + slice_index * 32, 32)],
            w_send.at[0], w_recv.at[0], partner,
        )

    def weight_along_y(k):
        rows = aligned(theirs + slice_index * 32, 32)
        return remote(wob.at[rows], wob.at[rows], w_send.at[1 + k], w_recv.at[1 + k], at_seq(ring_y[k]))

    def weight_along_x(k):
        rows = aligned(theirs + (core * 4 + x) * 128, 128)
        return remote(wob.at[rows], wob.at[rows], w_send.at[4 + k], w_recv.at[4 + k], at_seq(ring_x[k]))

    def weight_sibling():
        rows = aligned(theirs + core * 512, 512)
        return remote(wob.at[rows], wob.at[rows], w_send.at[7], w_recv.at[7], at_seq(sibling))

    def token_copy(i):
        rows = aligned(i * PART, PART)
        return remote(tok.at[rows], xbuf.at[head, rows], z_send.at[i], z_recv.at[i], partner)

    def token_arrival(i):
        rows = aligned(i * PART, PART)
        return remote(tok.at[rows], xbuf.at[other, rows], z_send.at[i], z_recv.at[i], partner)

    def flow(index, i, source, slot, target):
        return remote(
            kv.at[slot_rows(source, i)], kv.at[slot_rows(slot, i)], send.at[index, i], recv.at[index, i], at_seq(target)
        )

    def far(i):
        return flow(0, i, 0, 8, s + 8)

    def far_transit(i):
        column = lax.rem(i, 4)
        return remote(
            kv.at[slot_rows(0, i)], transit.at[lax.div(i, 4)], transit_send.at[i], transit_recv.at[lax.div(i, 4)],
            at_seq((16 + 4 * column + y) * 2 + core),
        )

    def onward(i):
        return remote(
            transit.at[lax.div(i, 4)], kv.at[slot_rows(8, i)], onward_send.at[lax.div(i, 4)], recv.at[0, i], at_seq(s - 8 * x)
        )

    def far_direct(i):
        return has_next & ((z == 1) | (x < 3) | (lax.rem(i, 4) == 0))

    def far_by_transit(i):
        return crosses & (lax.rem(i, 4) > 0)

    def onward_here(i):
        return (z == 1) & (x > 0) & (lax.rem(i, 4) == x)

    def up(i):
        return flow(1, i, jnp.where(y < 3, 0, 8), 2, seq_up)

    def down(i):
        return flow(2, i, jnp.where(y == 0, 0, 8), 6, seq_down)

    def second_up(i):
        return flow(3, i, 2, 4, seq_up)

    def second_down(i):
        return remote(
            kv.at[slot_rows(6, i)], kv.at[slot_rows(4, i)], send.at[4, i], recv.at[3, i], at_seq(seq_down)
        )

    def to_sibling(i, slot):
        target = slot + 1 - 2 * core
        lane = lax.div(target - 1, 2)
        return remote(
            kv.at[slot_rows(slot, i)], kv.at[slot_rows(target, i)], pair_send.at[lane, i], pair_recv.at[lane, i],
            at_seq(sibling),
        )

    up_own = y < 3
    up_relay = (y == 3) & has_prev
    down_own = y == 0
    down_relay = (y > 0) & has_prev
    second_up_valid = (y < 3) & (chip >= 1)
    second_down_valid = (y == 1) & has_prev

    weight_slice().start()
    for i in range(CHUNKS):
        token_copy(i).start()
    for load in loads[:4]:
        load.wait()
    weight_slice().wait_recv()
    for k in range(3):
        weight_along_y(k).start()

    def roped(values, rows):
        cos = cosine[rows]
        sin = sine[rows]
        leading = values[:, : HD // 2]
        trailing = values[:, HD // 2 :]
        return jnp.concatenate([leading * cos - trailing * sin, trailing * cos + leading * sin], axis=1).astype(BF16)

    def own(i):
        token_arrival(i).wait_recv()
        rows = aligned(i * PART, PART)
        first = xbuf[0, rows].astype(F32)
        second = xbuf[1, rows].astype(F32)
        squares = jnp.sum(first * first, axis=-1, keepdims=True) + jnp.sum(second * second, axis=-1, keepdims=True)
        scale = lax.rsqrt(squares / D + norm_epsilon)
        xn[:, :HALF] = (first * scale * gain[:, :HALF]).astype(BF16)
        xn[:, HALF:] = (second * scale * gain[:, HALF:]).astype(BF16)

        def key(j, carry):
            columns = aligned(j * HD, HD)
            product = jnp.dot(xn[...], wkb[:, columns], preferred_element_type=F32)
            kv[slot_rows(0, i), columns] = roped(product, rows)
            return carry

        def value(j, carry):
            product = jnp.dot(xn[...], wvb[:, aligned(j * HD, HD)], preferred_element_type=F32)
            kv[slot_rows(0, i), aligned(2 * HD + j * HD, HD)] = product.astype(BF16)
            return carry

        def query(j, carry):
            product = jnp.dot(xn[...], wqb[:, aligned(j * HD, HD)], preferred_element_type=F32)
            q[j, rows] = roped(product, rows)
            return carry

        lax.fori_loop(0, 2, value, 0)
        lax.fori_loop(0, 2, key, 0)
        when(far_direct(i), lambda: far(i).start())
        when(far_by_transit(i), lambda: far_transit(i).start())
        when(up_own, lambda: up(i).start())
        when(down_own, lambda: down(i).start())
        when(core == 0, lambda: to_sibling(i, 0).start())
        lax.fori_loop(0, 4, query, 0)

    def relay_onward(i):
        @pl.when(onward_here(i))
        def _():
            far_transit(i).wait_recv()
            onward(i).start()

    def relay_far(i):
        @pl.when(has_prev)
        def _():
            far(i).wait_recv()
            when(up_relay, lambda: up(i).start())
            when(down_relay, lambda: down(i).start())
            when(core == 1, lambda: to_sibling(i, 8).start())

    def relay_near(i):
        @pl.when(chip >= 1)
        def _():
            up(i).wait_recv()
            when(second_up_valid, lambda: second_up(i).start())
            to_sibling(i, 2).start()

        @pl.when(chip >= 3)
        def _():
            down(i).wait_recv()
            when(second_down_valid, lambda: second_down(i).start())
            to_sibling(i, 6).start()

    def relay_second(i):
        @pl.when(chip >= 2)
        def _():
            second_up(i).wait_recv()
            to_sibling(i, 4).start()

    def sibling_arrivals(first, last):
        def arrivals(i, carry):
            for lane in range(4):
                @pl.when(s >= 2 * lane + 1)
                def _():
                    rows = slot_rows(2 * lane + 1, i)
                    remote(kv.at[rows], kv.at[rows], pair_send.at[lane, i], pair_recv.at[lane, i], at_seq(sibling)).wait_recv()
            return carry

        lax.fori_loop(first, last, arrivals, 0)

    query_row = lax.rem(lax.broadcasted_iota(jnp.int32, (2 * TILE, TILE), 0), TILE)
    key_row = lax.broadcasted_iota(jnp.int32, (2 * TILE, TILE), 1)

    def attend(u, phase):
        group = lax.div(u, 2)
        tile = lax.rem(u, 2)
        key_columns = aligned(group * HD, HD)
        value_columns = aligned(2 * HD + group * HD, HD)
        query = q[pl.ds(2 * group, 2), aligned(tile * TILE, TILE)].reshape(2 * TILE, HD)

        def block(slot, mask):
            rows = aligned((SLOTS - 1 - slot) * ROWS + phase * TILE, TILE)
            scores = lax.dot_general(
                query, kv[rows, key_columns], (((1,), (1,)), ((), ())), preferred_element_type=F32
            )
            weights = jnp.exp2(EXP_SCALE * jnp.tanh(scores * SCORE_SCALE))
            if mask is not None:
                weights = jnp.where(mask, weights, 0.0)
            product = jnp.dot(weights.astype(BF16), kv[rows, value_columns], preferred_element_type=F32)
            return weights[:, :128] + weights[:, 128:], product

        def add(parts):
            partial, product = parts[0]
            for more_partial, more_product in parts[1:]:
                partial = partial + more_partial
                product = product + more_product
            den[u] += partial
            acc[u] += product

        if phase == 0:
            partial, product = block(0, key_row <= tile * TILE + query_row)
            den[u] = partial
            acc[u] = product

            @pl.when((tile == 0) & (s >= 8))
            def _():
                add([block(8, key_row > query_row)])
        else:
            @pl.when(tile == 1)
            def _():
                add([block(0, key_row <= query_row)])

            @pl.when(s >= 8)
            def _():
                add([block(8, TILE + key_row > tile * TILE + query_row)])

        count = jnp.minimum(7, s)
        groups = lax.div(count, 3)

        def triple(j, carry):
            add([block(1 + 3 * j + k, None) for k in range(3)])
            return carry

        def single(j, carry):
            add([block(1 + 3 * groups + j, None)])
            return carry

        lax.fori_loop(0, groups, triple, 0)
        lax.fori_loop(0, count - 3 * groups, single, 0)

    def step(t, carry):
        lag = 1 + ((z == 1) & (x == 0)).astype(jnp.int32)

        when(t < CHUNKS, lambda: own(t))
        when((t >= 1) & (t < CHUNKS + 1), lambda: relay_onward(t - 1))
        when((t >= lag) & (t < CHUNKS + lag), lambda: relay_far(t - lag))
        when((t >= lag + 1) & (t < CHUNKS + lag + 1), lambda: relay_near(t - lag - 1))
        when((t >= lag + 2) & (t < CHUNKS + lag + 2), lambda: relay_second(t - lag - 2))

        @pl.when(t == 0)
        def _():
            for k in range(3):
                weight_along_y(k).wait_recv()
            for k in range(3):
                weight_along_x(k).start()

        @pl.when(t == 3)
        def _():
            for k in range(3):
                weight_along_x(k).wait_recv()
            weight_sibling().start()

        @pl.when(t == CHUNKS - 1)
        def _():
            sibling_arrivals(0, CHUNKS // 2)

        when((t >= CHUNKS - 1) & (t < CHUNKS - 1 + UNITS), lambda: attend(t - CHUNKS + 1, 0))
        return carry

    lax.fori_loop(0, CHUNKS + 4, step, 0)
    sibling_arrivals(CHUNKS // 2, CHUNKS)
    weight_sibling().wait_recv()
    loads[4].wait()

    def unit_exchange(u):
        return remote(att.at[head, u], att.at[head, u], att_send.at[u], att_recv.at[u], partner)

    def unit_arrival(u):
        return remote(att.at[head, u], att.at[other, u], att_send.at[u], att_recv.at[u], partner)

    def project(u, which, fresh):
        group = lax.div(u, 2)
        tile = lax.rem(u, 2)
        rows = aligned(tile * TILE, TILE)

        def columns_of(j, carry):
            columns = aligned(j * 256, 256)
            product = jnp.dot(
                att[which, u], wob[aligned(which * 1024 + group * 512, 512), columns], preferred_element_type=F32
            )

            @pl.when(fresh)
            def _():
                branch[rows, columns] = product

            @pl.when(jnp.logical_not(fresh))
            def _():
                branch[rows, columns] += product

            return carry

        lax.fori_loop(0, HALF // 256, columns_of, 0)

    def second_phase(u, carry):
        attend(u, 1)
        denominator = jnp.sum(den[u], axis=-1, keepdims=True)
        attended = (acc[u] / denominator).astype(BF16)
        att[head, u] = jnp.concatenate([attended[:TILE], attended[TILE:]], axis=1)
        unit_exchange(u).start()
        project(u, head, u < 2)
        return carry

    lax.fori_loop(0, UNITS, second_phase, 0)

    diagonal = lax.broadcasted_iota(jnp.int32, (128, 128), 0) == lax.broadcasted_iota(jnp.int32, (128, 128), 1)

    def sums_copy(tile):
        return remote(sums.at[0, tile], sums.at[1, tile], sum_send.at[tile], sum_recv.at[tile], partner)

    def send_sums(tile):
        share = branch[aligned(tile * TILE, TILE)]
        totals = jnp.sum(share * share, axis=-1, keepdims=True)
        for block in range(2):
            spread = jnp.where(diagonal, totals[block * 128 : (block + 1) * 128], 0.0)
            sums[0, tile, block * 8 : (block + 1) * 8] = jnp.broadcast_to(jnp.sum(spread, axis=0, keepdims=True), (8, 128))
        sums_copy(tile).start()

    def output_copy(tile):
        rows = aligned(tile * TILE, TILE)
        return pltpu.make_async_copy(obuf.at[rows], out.at[rows], out_sem.at[tile])

    def finish(tile):
        sums_copy(tile).wait_recv()
        for block in range(2):
            rows = aligned(tile * TILE + block * 128, 128)
            both = sums[0, tile, block * 8 : block * 8 + 1] + sums[1, tile, block * 8 : block * 8 + 1]
            squares = jnp.sum(jnp.where(diagonal, both, 0.0), axis=1, keepdims=True)
            inverse = lax.rsqrt(squares / D + norm_epsilon)
            obuf[rows] = (xbuf[head, rows].astype(F32) + post[...] * branch[rows] * inverse).astype(BF16)
        output_copy(tile).start()

    def third_phase(u, carry):
        unit_arrival(u).wait_recv()
        project(u, other, u < 0)
        when(u >= 2, lambda: send_sums(u - 2))
        return carry

    lax.fori_loop(0, UNITS, third_phase, 0)
    finish(0)
    finish(1)

    def drain(i, carry):
        token_copy(i).wait_send()
        when(far_direct(i), lambda: far(i).wait_send())
        when(far_by_transit(i), lambda: far_transit(i).wait_send())
        when(onward_here(i), lambda: onward(i).wait_send())
        when(up_own | up_relay, lambda: up(i).wait_send())
        when(down_own | down_relay, lambda: down(i).wait_send())
        when(second_up_valid, lambda: second_up(i).wait_send())
        when(second_down_valid, lambda: second_down(i).wait_send())
        for slot in (0, 2, 4, 6, 8):
            sends = (slot <= s) & ((core == 0) if slot == 0 else (core == 1) if slot == 8 else (core >= 0))
            when(sends, lambda: to_sibling(i, slot).wait_send())
        return carry

    lax.fori_loop(0, CHUNKS, drain, 0)
    weight_slice().wait_send()
    for k in range(3):
        weight_along_y(k).wait_send()
        weight_along_x(k).wait_send()
    weight_sibling().wait_send()
    for u in range(UNITS):
        unit_exchange(u).wait_send()
    for tile in range(2):
        sums_copy(tile).wait_send()
        output_copy(tile).wait()


def local(tokens, pre_gain, query_weight, key_weight, value_weight, out_weight, post_gain):
    cosine, sine = rope_tables(ROWS)
    vmem = pl.BlockSpec(memory_space=pltpu.VMEM)
    hbm = pl.BlockSpec(memory_space=pl.ANY)
    dma = pltpu.SemaphoreType.DMA
    return pl.pallas_call(
        layer_kernel,
        out_shape=jax.ShapeDtypeStruct((ROWS, HALF), BF16),
        in_specs=[hbm, vmem, hbm, hbm, hbm, hbm, vmem, vmem, vmem],
        out_specs=hbm,
        scratch_shapes=[
            pltpu.VMEM((2, ROWS, HALF), BF16),
            pltpu.VMEM((PART, D), BF16),
            pltpu.VMEM((D, 4 * HD), BF16),
            pltpu.VMEM((D, 2 * HD), BF16),
            pltpu.VMEM((D, 2 * HD), BF16),
            pltpu.VMEM((2048, HALF), BF16),
            pltpu.VMEM((4, ROWS, HD), BF16),
            pltpu.VMEM((SLOTS * ROWS, 4 * HD), BF16),
            pltpu.VMEM((UNITS, 2 * TILE, HD), F32),
            pltpu.VMEM((UNITS, 2 * TILE, 128), F32),
            pltpu.VMEM((2, UNITS, TILE, 2 * HD), BF16),
            pltpu.VMEM((ROWS, HALF), F32),
            pltpu.VMEM((2, PART, 4 * HD), BF16),
            pltpu.VMEM((2, 2, 16, 128), F32),
            pltpu.VMEM((ROWS, HALF), BF16),
            dma((5,)),
            dma((CHUNKS,)),
            dma((CHUNKS,)),
            dma((5, CHUNKS)),
            dma((4, CHUNKS)),
            dma((4, CHUNKS)),
            dma((4, CHUNKS)),
            dma((CHUNKS,)),
            dma((2,)),
            dma((2,)),
            dma((8,)),
            dma((8,)),
            dma((UNITS,)),
            dma((UNITS,)),
            dma((2,)),
            dma((2,)),
            dma((2,)),
        ],
        compiler_params=pltpu.CompilerParams(
            collective_id=0, has_side_effects=True, vmem_limit_bytes=63 * 1024 * 1024
        ),
        name="layer",
    )(
        tokens, pre_gain[None, :], query_weight, key_weight, value_weight, out_weight,
        post_gain[None, :], cosine, sine,
    )


def solution(mesh):
    placed = (
        P("seq", "head"),
        P(),
        P(None, "head"),
        P(None, "head"),
        P(None, "head"),
        P("head", None),
        P("head"),
    )
    return jax.shard_map(
        local, mesh=mesh, in_specs=placed, out_specs=P("seq", "head"), check_vma=False
    )
```

```python
import math

import jax
import jax.numpy as jnp
import numpy as np
from jax import lax
from jax.experimental import pallas as pl
from jax.experimental.pallas import tpu as pltpu
from jax.sharding import PartitionSpec as P

D = 3584
HALF = 1792
HD = 256
ROWS = 512
CHUNKS = 8
PART = ROWS // CHUNKS
SLOTS = 9
TILE = 256
UNITS = 4
MESH = pl.DeviceIdType.MESH
F32 = jnp.float32
BF16 = jnp.bfloat16
softcap_limit = 50.0
rope_base = 10000.0
norm_epsilon = 1e-06
EXP_SCALE = softcap_limit * math.log2(math.e)
SCORE_SCALE = HD ** (-0.5) / softcap_limit


def rope_rows():
    frequency = rope_base ** (-2.0 * np.arange(HD // 2) / HD)
    angles = np.arange(ROWS)[:, None] * frequency[None, :]
    table = np.stack([np.cos(angles), np.sin(angles)])
    return table.astype(np.float32), np.broadcast_to(frequency, (8, HD // 2)).astype(np.float32)


def aligned(start, size, step=None):
    return pl.ds(pl.multiple_of(start, step or size), size)


def slot_rows(slot, chunk):
    return aligned((SLOTS - 1 - slot) * ROWS + chunk * PART, PART)


def when(condition, action):
    pl.when(condition)(action)


def layer_kernel(
    tok, gain, wq, wk, wv, wo, post, turns, frequency, out,
    xbuf, xn, wqb, wkb, wvb, wob, q, kv, acc, den, att, branch, transit, sums, obuf, cosine, sine,
    load_sem, z_send, z_recv, send, recv, pair_send, pair_recv,
    transit_send, transit_recv, onward_send, w_send, w_recv, att_send, att_recv, sum_send, sum_recv, out_sem,
):
    s = lax.axis_index("seq")
    head = lax.axis_index("head")
    core = lax.rem(s, 2)
    chip = lax.div(s, 2)
    y = lax.rem(chip, 4)
    x = lax.rem(lax.div(chip, 4), 4)
    z = lax.div(chip, 16)
    other = 1 - head
    seq_up = s + jnp.where(y < 3, 2, -6)
    seq_down = s + jnp.where(y > 0, -2, 6)
    sibling = s + 1 - 2 * core
    has_next = chip < 28
    has_prev = chip >= 4
    crosses = (z == 0) & (x == 3)
    ring_y = [s + 2 * (lax.rem(y + k, 4) - y) for k in (1, 2, 3)]
    ring_x = [s + 8 * (lax.rem(x + k, 4) - x) for k in (1, 2, 3)]

    def at_seq(target):
        return (target, head)

    partner = (s, other)

    def remote(source, target, send_sem, recv_sem, device):
        return pltpu.make_async_remote_copy(
            src_ref=source, dst_ref=target, send_sem=send_sem, recv_sem=recv_sem,
            device_id=device, device_id_type=MESH,
        )

    own_columns = aligned(head * HALF, HALF, 128)
    other_columns = aligned(other * HALF, HALF, 128)
    loads = [
        pltpu.make_async_copy(tok, xbuf.at[head], load_sem.at[0]),
        pltpu.make_async_copy(wv, wvb, load_sem.at[1]),
        pltpu.make_async_copy(wk, wkb, load_sem.at[2]),
        pltpu.make_async_copy(wq, wqb, load_sem.at[3]),
        pltpu.make_async_copy(wo.at[:, own_columns], wob.at[aligned(head * 1024, 1024)], load_sem.at[4]),
    ]
    for load in loads:
        load.start()

    barrier = pltpu.get_barrier_semaphore()

    def greet(device):
        pl.semaphore_signal(barrier, inc=1, device_id=device, device_id_type=MESH)

    greet(partner)
    greet(at_seq(sibling))
    for target in ring_y + ring_x:
        greet(at_seq(target))

    @pl.when(z == 1)
    def _():
        greet(at_seq((12 + y) * 2 + core))

    @pl.when(crosses)
    def _():
        for column in range(4):
            greet(at_seq((16 + 4 * column + y) * 2 + core))

    pl.semaphore_wait(barrier, 8 + z + 4 * crosses.astype(jnp.int32))

    slice_index = (core * 4 + x) * 4 + y
    mine = head * 1024
    theirs = other * 1024

    def weight_slice():
        return remote(
            wo.at[aligned(slice_index * 32, 32), other_columns], wob.at[aligned(mine + slice_index * 32, 32)],
            w_send.at[0], w_recv.at[0], partner,
        )

    def weight_along_y(k):
        rows = aligned(theirs + slice_index * 32, 32)
        return remote(wob.at[rows], wob.at[rows], w_send.at[1 + k], w_recv.at[1 + k], at_seq(ring_y[k]))

    def weight_along_x(hop):
        column = lax.rem(x + 1, 4) if hop == 1 else x
        rows = aligned(theirs + (core * 4 + column) * 128, 128)
        return remote(wob.at[rows], wob.at[rows], w_send.at[4 + hop], w_recv.at[4 + hop], at_seq(ring_x[0 if hop == 2 else 2]))

    def weight_sibling():
        rows = aligned(theirs + core * 512, 512)
        return remote(wob.at[rows], wob.at[rows], w_send.at[7], w_recv.at[7], at_seq(sibling))

    def token_copy(i):
        rows = aligned(i * PART, PART)
        return remote(tok.at[rows], xbuf.at[head, rows], z_send.at[i], z_recv.at[i], partner)

    def token_arrival(i):
        rows = aligned(i * PART, PART)
        return remote(tok.at[rows], xbuf.at[other, rows], z_send.at[i], z_recv.at[i], partner)

    def flow(index, i, source, slot, target):
        return remote(
            kv.at[slot_rows(source, i)], kv.at[slot_rows(slot, i)], send.at[index, i], recv.at[index, i], at_seq(target)
        )

    def far(i):
        return flow(0, i, 0, 8, s + 8)

    def far_transit(i):
        column = lax.rem(i + 1, 4)
        return remote(
            kv.at[slot_rows(0, i)], transit.at[lax.div(i, 4)], transit_send.at[i], transit_recv.at[lax.div(i, 4)],
            at_seq((16 + 4 * column + y) * 2 + core),
        )

    def onward(i):
        return remote(
            transit.at[lax.div(i, 4)], kv.at[slot_rows(8, i)], onward_send.at[lax.div(i, 4)], recv.at[0, i], at_seq(s - 8 * x)
        )

    def far_direct(i):
        return has_next & ((z == 1) | (x < 3) | (lax.rem(i, 4) == 3))

    def far_by_transit(i):
        return crosses & (lax.rem(i, 4) < 3)

    def onward_here(i):
        return (z == 1) & (x > 0) & (lax.rem(i, 4) == x - 1)

    def up(i):
        return flow(1, i, jnp.where(y < 3, 0, 8), 2, seq_up)

    def down(i):
        return flow(2, i, jnp.where(y == 0, 0, 8), 6, seq_down)

    def second_up(i):
        return flow(3, i, 2, 4, seq_up)

    def second_down(i):
        return remote(
            kv.at[slot_rows(6, i)], kv.at[slot_rows(4, i)], send.at[4, i], recv.at[3, i], at_seq(seq_down)
        )

    def to_sibling(i, slot):
        target = slot + 1 - 2 * core
        lane = lax.div(target - 1, 2)
        return remote(
            kv.at[slot_rows(slot, i)], kv.at[slot_rows(target, i)], pair_send.at[lane, i], pair_recv.at[lane, i],
            at_seq(sibling),
        )

    up_own = y < 3
    up_relay = (y == 3) & has_prev
    down_own = y == 0
    down_relay = (y > 0) & has_prev
    second_up_valid = (y < 3) & (chip >= 1)
    second_down_valid = (y == 1) & has_prev

    weight_slice().start()
    for i in range(CHUNKS):
        token_copy(i).start()
    base = jnp.sum(jnp.where(lax.broadcasted_iota(jnp.int32, (8, HD // 2), 0) == 0, frequency[...], 0.0), axis=0, keepdims=True)
    base = base * (s * ROWS).astype(F32)
    base_cos = jnp.cos(base)
    base_sin = jnp.sin(base)
    cosine[...] = base_cos * turns[0] - base_sin * turns[1]
    sine[...] = base_sin * turns[0] + base_cos * turns[1]
    for load in loads[:3]:
        load.wait()
    weight_slice().wait_recv()
    for k in range(3):
        weight_along_y(k).start()

    def roped(values, rows):
        cos = cosine[rows]
        sin = sine[rows]
        leading = values[:, : HD // 2]
        trailing = values[:, HD // 2 :]
        return jnp.concatenate([leading * cos - trailing * sin, trailing * cos + leading * sin], axis=1).astype(BF16)

    def own(i):
        token_arrival(i).wait_recv()
        rows = aligned(i * PART, PART)
        first = xbuf[0, rows].astype(F32)
        second = xbuf[1, rows].astype(F32)
        squares = jnp.sum(first * first, axis=-1, keepdims=True) + jnp.sum(second * second, axis=-1, keepdims=True)
        scale = lax.rsqrt(squares / D + norm_epsilon)
        xn[rows, :HALF] = (first * scale * gain[:HALF][None, :]).astype(BF16)
        xn[rows, HALF:] = (second * scale * gain[HALF:][None, :]).astype(BF16)

        def value(j, carry):
            product = jnp.dot(xn[rows], wvb[:, aligned(j * HD, HD)], preferred_element_type=F32)
            kv[slot_rows(0, i), aligned(2 * HD + j * HD, HD)] = product.astype(BF16)
            return carry

        def key(j, carry):
            columns = aligned(j * HD, HD)
            product = jnp.dot(xn[rows], wkb[:, columns], preferred_element_type=F32)
            kv[slot_rows(0, i), columns] = roped(product, rows)
            return carry

        lax.fori_loop(0, 2, value, 0)
        lax.fori_loop(0, 2, key, 0)
        when(far_direct(i), lambda: far(i).start())
        when(far_by_transit(i), lambda: far_transit(i).start())
        when(up_own, lambda: up(i).start())
        when(down_own, lambda: down(i).start())
        when(core == 0, lambda: to_sibling(i, 0).start())

    def queries(tile):
        rows = aligned(tile * TILE, TILE)

        def query(j, carry):
            product = jnp.dot(xn[rows], wqb[:, aligned(j * HD, HD)], preferred_element_type=F32)
            q[j, rows] = roped(product, rows)
            return carry

        lax.fori_loop(0, 4, query, 0)

    def relay_onward(i):
        @pl.when(onward_here(i))
        def _():
            far_transit(i).wait_recv()
            onward(i).start()

    def relay_far(i):
        @pl.when(has_prev)
        def _():
            far(i).wait_recv()
            when(up_relay, lambda: up(i).start())
            when(down_relay, lambda: down(i).start())
            when(core == 1, lambda: to_sibling(i, 8).start())

    def relay_near(i):
        @pl.when(chip >= 1)
        def _():
            up(i).wait_recv()
            when(second_up_valid, lambda: second_up(i).start())
            to_sibling(i, 2).start()

        @pl.when(chip >= 3)
        def _():
            down(i).wait_recv()
            when(second_down_valid, lambda: second_down(i).start())
            to_sibling(i, 6).start()

    def relay_second(i):
        @pl.when(chip >= 2)
        def _():
            second_up(i).wait_recv()
            to_sibling(i, 4).start()

    def sibling_arrivals(first, last):
        def arrivals(i, carry):
            for lane in range(4):
                @pl.when(s >= 2 * lane + 1)
                def _():
                    rows = slot_rows(2 * lane + 1, i)
                    remote(kv.at[rows], kv.at[rows], pair_send.at[lane, i], pair_recv.at[lane, i], at_seq(sibling)).wait_recv()
            return carry

        lax.fori_loop(first, last, arrivals, 0)

    query_row = lax.rem(lax.broadcasted_iota(jnp.int32, (2 * TILE, TILE), 0), TILE)
    key_row = lax.broadcasted_iota(jnp.int32, (2 * TILE, TILE), 1)

    def attend(group, tile, phase):
        u = 2 * tile + group
        key_columns = aligned(group * HD, HD)
        value_columns = aligned(2 * HD + group * HD, HD)
        query = q[pl.ds(2 * group, 2), tile * TILE : (tile + 1) * TILE].reshape(2 * TILE, HD)

        def block(slot, mask):
            rows = aligned((SLOTS - 1 - slot) * ROWS + phase * TILE, TILE)
            scores = lax.dot_general(
                query, kv[rows, key_columns], (((1,), (1,)), ((), ())), preferred_element_type=F32
            )
            weights = jnp.exp2(EXP_SCALE * jnp.tanh(scores * SCORE_SCALE))
            if mask is not None:
                weights = jnp.where(mask, weights, 0.0)
            product = jnp.dot(weights.astype(BF16), kv[rows, value_columns], preferred_element_type=F32)
            return weights[:, :128] + weights[:, 128:], product

        def add(parts, fresh):
            partial, product = parts[0]
            for more_partial, more_product in parts[1:]:
                partial = partial + more_partial
                product = product + more_product
            if fresh:
                den[u] = partial
                acc[u] = product
            else:
                den[u] += partial
                acc[u] += product

        def causal():
            return block(0, (key_row <= query_row) if tile == phase else None)

        def edge():
            return block(8, (key_row > query_row) if tile == phase else None)

        has_causal = phase <= tile
        has_edge = phase >= tile

        @pl.when(s >= 8)
        def _():
            parts = [block(slot, None) for slot in range(1, 8)]
            if has_causal:
                parts.insert(0, causal())
            if has_edge:
                parts.append(edge())
            add(parts, phase == 0)

        @pl.when(s < 8)
        def _():
            if phase == 0:
                add([causal()], True)
            elif has_causal:
                add([causal()], False)

            def single(j, carry):
                add([block(1 + j, None)], False)
                return carry

            lax.fori_loop(0, jnp.minimum(7, s), single, 0)

    lag = 1 + ((z == 1) & (x == 0)).astype(jnp.int32)
    first_attend = lag + 5

    def relayed(t, hops):
        return jnp.where(t >= CHUNKS + hops, CHUNKS, jnp.clip(t - lag + 1 - hops, 0, CHUNKS))

    def relay(t, hops, action):
        def one(i, carry):
            action(i)
            return carry

        lax.fori_loop(relayed(t - 1, hops), relayed(t, hops), one, 0)

    def step(t, carry):
        when(t < CHUNKS, lambda: own(t))
        when((t >= 1) & (t < CHUNKS + 1), lambda: relay_onward(t - 1))
        relay(t, 0, relay_far)
        relay(t, 1, relay_near)
        relay(t, 2, relay_second)

        @pl.when(t == 0)
        def _():
            for k in range(3):
                weight_along_y(k).wait_recv()
            weight_along_x(0).start()
            loads[3].wait()

        @pl.when(t == 4)
        def _():
            weight_along_x(0).wait_recv()
            weight_along_x(1).start()

        when(t == CHUNKS, lambda: weight_along_x(2).start())
        when(t == 3, lambda: queries(0))
        when(t == CHUNKS - 1, lambda: queries(1))
        when(t == first_attend, lambda: sibling_arrivals(0, CHUNKS // 2))
        when((t >= first_attend) & (t < first_attend + 2), lambda: attend(t - first_attend, 0, 0))
        when((t >= first_attend + 2) & (t < first_attend + 4), lambda: attend(t - first_attend - 2, 1, 0))
        return carry

    lax.fori_loop(0, CHUNKS + 3, step, 0)
    for hop in (1, 2):
        weight_along_x(hop).wait_recv()
    weight_sibling().start()
    sibling_arrivals(CHUNKS // 2, CHUNKS)
    loads[4].wait()

    def unit_exchange(u):
        return remote(att.at[head, u], att.at[head, u], att_send.at[u], att_recv.at[u], partner)

    def unit_arrival(u):
        return remote(att.at[head, u], att.at[other, u], att_send.at[u], att_recv.at[u], partner)

    def project(tile, which, groups, fresh):
        rows = slice(tile * TILE, (tile + 1) * TILE)

        def columns_of(j, carry):
            columns = aligned(j * 896, 896)
            product = None
            for group in groups:
                term = jnp.dot(
                    att[which, 2 * tile + group], wob[aligned(which * 1024 + group * 512, 512), columns],
                    preferred_element_type=F32,
                )
                product = term if product is None else product + term
            if fresh:
                branch[rows, columns] = product
            else:
                branch[rows, columns] += product
            return carry

        lax.fori_loop(0, HALF // 896, columns_of, 0)

    for tile in range(2):
        def second_phase(group, carry):
            u = 2 * tile + group
            attend(group, tile, 1)
            denominator = jnp.sum(den[u], axis=-1, keepdims=True)
            attended = (acc[u] / denominator).astype(BF16)
            att[head, u] = jnp.concatenate([attended[:TILE], attended[TILE:]], axis=1)
            unit_exchange(u).start()
            return carry

        lax.fori_loop(0, 2, second_phase, 0)
        if tile == 1:
            for part in range(2):
                project(part, head, (0, 1), True)

    diagonal = lax.broadcasted_iota(jnp.int32, (128, 128), 0) == lax.broadcasted_iota(jnp.int32, (128, 128), 1)

    def sums_copy(tile):
        return remote(sums.at[0, tile], sums.at[1, tile], sum_send.at[tile], sum_recv.at[tile], partner)

    def send_sums(tile):
        share = branch[aligned(tile * TILE, TILE)]
        totals = jnp.sum(share * share, axis=-1, keepdims=True)
        for block in range(2):
            spread = jnp.where(diagonal, totals[block * 128 : (block + 1) * 128], 0.0)
            sums[0, tile, block * 8 : (block + 1) * 8] = jnp.broadcast_to(jnp.sum(spread, axis=0, keepdims=True), (8, 128))
        sums_copy(tile).start()

    def output_copy(tile):
        rows = aligned(tile * TILE, TILE)
        return pltpu.make_async_copy(obuf.at[rows], out.at[rows], out_sem.at[tile])

    def finish(tile):
        sums_copy(tile).wait_recv()
        for block in range(2):
            rows = aligned(tile * TILE + block * 128, 128)
            both = sums[0, tile, block * 8 : block * 8 + 1] + sums[1, tile, block * 8 : block * 8 + 1]
            squares = jnp.sum(jnp.where(diagonal, both, 0.0), axis=1, keepdims=True)
            inverse = lax.rsqrt(squares / D + norm_epsilon)
            obuf[rows] = (xbuf[head, rows].astype(F32) + post[...][None, :] * branch[rows] * inverse).astype(BF16)
        output_copy(tile).start()

    weight_sibling().wait_recv()
    unit_arrival(0).wait_recv()
    unit_arrival(1).wait_recv()
    project(0, other, (0, 1), False)
    send_sums(0)
    unit_arrival(2).wait_recv()
    project(1, other, (0,), False)
    finish(0)
    unit_arrival(3).wait_recv()
    project(1, other, (1,), False)
    send_sums(1)
    finish(1)

    def drain(i, carry):
        token_copy(i).wait_send()
        when(far_direct(i), lambda: far(i).wait_send())
        when(far_by_transit(i), lambda: far_transit(i).wait_send())
        when(onward_here(i), lambda: onward(i).wait_send())
        when(up_own | up_relay, lambda: up(i).wait_send())
        when(down_own | down_relay, lambda: down(i).wait_send())
        when(second_up_valid, lambda: second_up(i).wait_send())
        when(second_down_valid, lambda: second_down(i).wait_send())
        for slot in (0, 2, 4, 6, 8):
            sends = (slot <= s) & ((core == 0) if slot == 0 else (core == 1) if slot == 8 else (core >= 0))
            when(sends, lambda: to_sibling(i, slot).wait_send())
        return carry

    lax.fori_loop(0, CHUNKS, drain, 0)
    weight_slice().wait_send()
    for k in range(3):
        weight_along_y(k).wait_send()
        weight_along_x(k).wait_send()
    weight_sibling().wait_send()
    for u in range(UNITS):
        unit_exchange(u).wait_send()
    for tile in range(2):
        sums_copy(tile).wait_send()
        output_copy(tile).wait()


def local(tokens, pre_gain, query_weight, key_weight, value_weight, out_weight, post_gain):
    turns, frequency = rope_rows()
    vmem = pl.BlockSpec(memory_space=pltpu.VMEM)
    hbm = pl.BlockSpec(memory_space=pl.ANY)
    dma = pltpu.SemaphoreType.DMA
    return pl.pallas_call(
        layer_kernel,
        out_shape=jax.ShapeDtypeStruct((ROWS, HALF), BF16),
        in_specs=[hbm, vmem, hbm, hbm, hbm, hbm, vmem, vmem, vmem],
        out_specs=hbm,
        scratch_shapes=[
            pltpu.VMEM((2, ROWS, HALF), BF16),
            pltpu.VMEM((ROWS, D), BF16),
            pltpu.VMEM((D, 4 * HD), BF16),
            pltpu.VMEM((D, 2 * HD), BF16),
            pltpu.VMEM((D, 2 * HD), BF16),
            pltpu.VMEM((2048, HALF), BF16),
            pltpu.VMEM((4, ROWS, HD), BF16),
            pltpu.VMEM((SLOTS * ROWS, 4 * HD), BF16),
            pltpu.VMEM((UNITS, 2 * TILE, HD), F32),
            pltpu.VMEM((UNITS, 2 * TILE, 128), F32),
            pltpu.VMEM((2, UNITS, TILE, 2 * HD), BF16),
            pltpu.VMEM((ROWS, HALF), F32),
            pltpu.VMEM((2, PART, 4 * HD), BF16),
            pltpu.VMEM((2, 2, 16, 128), F32),
            pltpu.VMEM((ROWS, HALF), BF16),
            pltpu.VMEM((ROWS, HD // 2), F32),
            pltpu.VMEM((ROWS, HD // 2), F32),
            dma((5,)),
            dma((CHUNKS,)),
            dma((CHUNKS,)),
            dma((5, CHUNKS)),
            dma((4, CHUNKS)),
            dma((4, CHUNKS)),
            dma((4, CHUNKS)),
            dma((CHUNKS,)),
            dma((2,)),
            dma((2,)),
            dma((8,)),
            dma((8,)),
            dma((UNITS,)),
            dma((UNITS,)),
            dma((2,)),
            dma((2,)),
            dma((2,)),
        ],
        compiler_params=pltpu.CompilerParams(
            collective_id=0, has_side_effects=True, vmem_limit_bytes=63 * 1024 * 1024
        ),
        name="layer",
    )(
        tokens, pre_gain, query_weight, key_weight, value_weight, out_weight,
        post_gain, turns, frequency,
    )


def solution(mesh):
    placed = (
        P("seq", "head"),
        P(),
        P(None, "head"),
        P(None, "head"),
        P(None, "head"),
        P("head", None),
        P("head"),
    )
    return jax.shard_map(
        local, mesh=mesh, in_specs=placed, out_specs=P("seq", "head"), check_vma=False
    )
```

```python
import math

import jax
import jax.numpy as jnp
import numpy as np
from jax import lax
from jax.experimental import pallas as pl
from jax.experimental.pallas import tpu as pltpu
from jax.sharding import PartitionSpec as P

D = 3584
HALF = 1792
HD = 256
ROWS = 512
CHUNKS = 8
PART = ROWS // CHUNKS
SLOTS = 9
TILE = 256
UNITS = 4
MESH = pl.DeviceIdType.MESH
F32 = jnp.float32
BF16 = jnp.bfloat16
softcap_limit = 50.0
rope_base = 10000.0
norm_epsilon = 1e-06
EXP_SCALE = softcap_limit * math.log2(math.e)
SCORE_SCALE = HD ** (-0.5) / softcap_limit


def rope_rows():
    frequency = rope_base ** (-2.0 * np.arange(HD // 2) / HD)
    angles = np.arange(ROWS)[:, None] * frequency[None, :]
    table = np.stack([np.cos(angles), np.sin(angles)])
    return table.astype(np.float32), np.broadcast_to(frequency, (8, HD // 2)).astype(np.float32)


def aligned(start, size, step=None):
    return pl.ds(pl.multiple_of(start, step or size), size)


def slot_rows(slot, chunk):
    return aligned((SLOTS - 1 - slot) * ROWS + chunk * PART, PART)


def when(condition, action):
    pl.when(condition)(action)


def layer_kernel(
    tok, gain, wq, wk, wv, wo, post, turns, frequency, out,
    xbuf, xn, wqb, wkb, wvb, wob, q, kv, acc, den, att, branch, transit, sums, obuf, cosine, sine,
    load_sem, z_send, z_recv, send, recv, pair_send, pair_recv,
    transit_send, transit_recv, onward_send, w_send, w_recv, att_send, att_recv, sum_send, sum_recv, out_sem,
):
    s = lax.axis_index("seq")
    head = lax.axis_index("head")
    core = lax.rem(s, 2)
    chip = lax.div(s, 2)
    y = lax.rem(chip, 4)
    x = lax.rem(lax.div(chip, 4), 4)
    z = lax.div(chip, 16)
    other = 1 - head
    seq_up = s + jnp.where(y < 3, 2, -6)
    seq_down = s + jnp.where(y > 0, -2, 6)
    sibling = s + 1 - 2 * core
    has_next = chip < 28
    has_prev = chip >= 4
    crosses = (z == 0) & (x == 3)
    ring_y = [s + 2 * (lax.rem(y + k, 4) - y) for k in (1, 2, 3)]
    ring_x = [s + 8 * (lax.rem(x + k, 4) - x) for k in (1, 2, 3)]

    def at_seq(target):
        return (target, head)

    partner = (s, other)
    weight_partner = (s + 32 - 64 * z, other)

    def remote(source, target, send_sem, recv_sem, device):
        return pltpu.make_async_remote_copy(
            src_ref=source, dst_ref=target, send_sem=send_sem, recv_sem=recv_sem,
            device_id=device, device_id_type=MESH,
        )

    own_columns = aligned(head * HALF, HALF, 128)
    other_columns = aligned(other * HALF, HALF, 128)
    loads = [
        pltpu.make_async_copy(tok, xbuf.at[head], load_sem.at[0]),
        pltpu.make_async_copy(wv, wvb, load_sem.at[1]),
        pltpu.make_async_copy(wk, wkb, load_sem.at[2]),
        pltpu.make_async_copy(wq, wqb, load_sem.at[3]),
        pltpu.make_async_copy(wo.at[:, own_columns], wob.at[aligned(head * 1024, 1024)], load_sem.at[4]),
    ]
    for load in loads:
        load.start()

    barrier = pltpu.get_barrier_semaphore()

    def greet(device):
        pl.semaphore_signal(barrier, inc=1, device_id=device, device_id_type=MESH)

    greet(partner)
    greet(weight_partner)
    greet(at_seq(sibling))
    for target in ring_y + ring_x:
        greet(at_seq(target))

    @pl.when((z == 1) & (x < 3))
    def _():
        greet(at_seq((12 + y) * 2 + core))

    @pl.when(crosses)
    def _():
        for column in range(3):
            greet(at_seq((16 + 4 * column + y) * 2 + core))

    pl.semaphore_wait(barrier, 9 + ((z == 1) & (x < 3)).astype(jnp.int32) + 3 * crosses.astype(jnp.int32))

    slice_index = (core * 4 + x) * 4 + y
    mine = head * 1024
    theirs = other * 1024

    def weight_slice():
        return remote(
            wo.at[aligned(slice_index * 32, 32), other_columns], wob.at[aligned(mine + slice_index * 32, 32)],
            w_send.at[0], w_recv.at[0], weight_partner,
        )

    def weight_along_y(k):
        rows = aligned(theirs + slice_index * 32, 32)
        return remote(wob.at[rows], wob.at[rows], w_send.at[1 + k], w_recv.at[1 + k], at_seq(ring_y[k]))

    def weight_along_x(hop):
        column = lax.rem(x + 1, 4) if hop == 1 else x
        rows = aligned(theirs + (core * 4 + column) * 128, 128)
        return remote(wob.at[rows], wob.at[rows], w_send.at[4 + hop], w_recv.at[4 + hop], at_seq(ring_x[0 if hop == 2 else 2]))

    def weight_sibling():
        rows = aligned(theirs + core * 512, 512)
        return remote(wob.at[rows], wob.at[rows], w_send.at[7], w_recv.at[7], at_seq(sibling))

    def token_copy(i):
        rows = aligned(i * PART, PART)
        return remote(tok.at[rows], xbuf.at[head, rows], z_send.at[i], z_recv.at[i], partner)

    def token_arrival(i):
        rows = aligned(i * PART, PART)
        return remote(tok.at[rows], xbuf.at[other, rows], z_send.at[i], z_recv.at[i], partner)

    def flow(index, i, source, slot, target):
        return remote(
            kv.at[slot_rows(source, i)], kv.at[slot_rows(slot, i)], send.at[index, i], recv.at[index, i], at_seq(target)
        )

    def far(i):
        return flow(0, i, 0, 8, s + 8)

    def far_transit(i):
        column = lax.rem(i + 2, 3)
        return remote(
            kv.at[slot_rows(0, i)], transit.at[lax.div(i, 3)], transit_send.at[i], transit_recv.at[lax.div(i, 3)],
            at_seq((16 + 4 * column + y) * 2 + core),
        )

    def onward(i):
        return remote(
            transit.at[lax.div(i, 3)], kv.at[slot_rows(8, i)], onward_send.at[lax.div(i, 3)], recv.at[0, i], at_seq(s - 8 * x)
        )

    def far_direct(i):
        return has_next & ((z == 1) | (x < 3) | (lax.rem(i, 3) == 1))

    def far_by_transit(i):
        return crosses & (lax.rem(i, 3) != 1)

    def onward_here(i):
        return (z == 1) & (x > 0) & (lax.rem(i + 2, 3) == x)

    def up(i):
        return flow(1, i, jnp.where(y < 3, 0, 8), 2, seq_up)

    def down(i):
        return flow(2, i, jnp.where(y == 0, 0, 8), 6, seq_down)

    def second_up(i):
        return flow(3, i, 2, 4, seq_up)

    def second_down(i):
        return remote(
            kv.at[slot_rows(6, i)], kv.at[slot_rows(4, i)], send.at[4, i], recv.at[3, i], at_seq(seq_down)
        )

    def to_sibling(i, slot):
        target = slot + 1 - 2 * core
        lane = lax.div(target - 1, 2)
        return remote(
            kv.at[slot_rows(slot, i)], kv.at[slot_rows(target, i)], pair_send.at[lane, i], pair_recv.at[lane, i],
            at_seq(sibling),
        )

    up_own = y < 3
    up_relay = (y == 3) & has_prev
    down_own = y == 0
    down_relay = (y > 0) & has_prev
    second_up_valid = (y < 3) & (chip >= 1)
    second_down_valid = (y == 1) & has_prev

    weight_slice().start()
    for i in range(CHUNKS):
        token_copy(i).start()
    base = jnp.sum(jnp.where(lax.broadcasted_iota(jnp.int32, (8, HD // 2), 0) == 0, frequency[...], 0.0), axis=0, keepdims=True)
    base = base * (s * ROWS).astype(F32)
    base_cos = jnp.cos(base)
    base_sin = jnp.sin(base)
    cosine[...] = base_cos * turns[0] - base_sin * turns[1]
    sine[...] = base_sin * turns[0] + base_cos * turns[1]
    for load in loads[:3]:
        load.wait()
    weight_slice().wait_recv()
    for k in range(3):
        weight_along_y(k).start()

    def roped(values, rows):
        cos = cosine[rows]
        sin = sine[rows]
        leading = values[:, : HD // 2]
        trailing = values[:, HD // 2 :]
        return jnp.concatenate([leading * cos - trailing * sin, trailing * cos + leading * sin], axis=1).astype(BF16)

    def own(i):
        token_arrival(i).wait_recv()
        rows = aligned(i * PART, PART)
        first = xbuf[0, rows].astype(F32)
        second = xbuf[1, rows].astype(F32)
        squares = jnp.sum(first * first, axis=-1, keepdims=True) + jnp.sum(second * second, axis=-1, keepdims=True)
        scale = lax.rsqrt(squares / D + norm_epsilon)
        xn[rows, :HALF] = (first * scale * gain[:HALF][None, :]).astype(BF16)
        xn[rows, HALF:] = (second * scale * gain[HALF:][None, :]).astype(BF16)

        def value(j, carry):
            product = jnp.dot(xn[rows], wvb[:, aligned(j * HD, HD)], preferred_element_type=F32)
            kv[slot_rows(0, i), aligned(2 * HD + j * HD, HD)] = product.astype(BF16)
            return carry

        def key(j, carry):
            columns = aligned(j * HD, HD)
            product = jnp.dot(xn[rows], wkb[:, columns], preferred_element_type=F32)
            kv[slot_rows(0, i), columns] = roped(product, rows)
            return carry

        lax.fori_loop(0, 2, value, 0)
        lax.fori_loop(0, 2, key, 0)
        when(far_direct(i), lambda: far(i).start())
        when(far_by_transit(i), lambda: far_transit(i).start())
        when(up_own, lambda: up(i).start())
        when(down_own, lambda: down(i).start())
        when(core == 0, lambda: to_sibling(i, 0).start())

    def queries(tile):
        rows = aligned(tile * TILE, TILE)

        def query(j, carry):
            product = jnp.dot(xn[rows], wqb[:, aligned(j * HD, HD)], preferred_element_type=F32)
            q[j, rows] = roped(product, rows)
            return carry

        lax.fori_loop(0, 4, query, 0)

    def relay_onward(i):
        @pl.when(onward_here(i))
        def _():
            far_transit(i).wait_recv()
            onward(i).start()

    def relay_far(i):
        @pl.when(has_prev)
        def _():
            far(i).wait_recv()
            when(up_relay, lambda: up(i).start())
            when(down_relay, lambda: down(i).start())
            when(core == 1, lambda: to_sibling(i, 8).start())

    def relay_near(i):
        @pl.when(chip >= 1)
        def _():
            up(i).wait_recv()
            when(second_up_valid, lambda: second_up(i).start())
            to_sibling(i, 2).start()

        @pl.when(chip >= 3)
        def _():
            down(i).wait_recv()
            when(second_down_valid, lambda: second_down(i).start())
            to_sibling(i, 6).start()

    def relay_second(i):
        @pl.when(chip >= 2)
        def _():
            second_up(i).wait_recv()
            to_sibling(i, 4).start()

    def sibling_arrivals(first, last):
        def arrivals(i, carry):
            for lane in range(4):
                @pl.when(s >= 2 * lane + 1)
                def _():
                    rows = slot_rows(2 * lane + 1, i)
                    remote(kv.at[rows], kv.at[rows], pair_send.at[lane, i], pair_recv.at[lane, i], at_seq(sibling)).wait_recv()
            return carry

        lax.fori_loop(first, last, arrivals, 0)

    query_row = lax.rem(lax.broadcasted_iota(jnp.int32, (2 * TILE, TILE), 0), TILE)
    key_row = lax.broadcasted_iota(jnp.int32, (2 * TILE, TILE), 1)

    def attend(group, tile, phase):
        u = 2 * tile + group
        key_columns = aligned(group * HD, HD)
        value_columns = aligned(2 * HD + group * HD, HD)
        query = q[pl.ds(2 * group, 2), tile * TILE : (tile + 1) * TILE].reshape(2 * TILE, HD)

        def block(slot, mask):
            rows = aligned((SLOTS - 1 - slot) * ROWS + phase * TILE, TILE)
            scores = lax.dot_general(
                query, kv[rows, key_columns], (((1,), (1,)), ((), ())), preferred_element_type=F32
            )
            weights = jnp.exp2(EXP_SCALE * jnp.tanh(scores * SCORE_SCALE))
            if mask is not None:
                weights = jnp.where(mask, weights, 0.0)
            product = jnp.dot(weights.astype(BF16), kv[rows, value_columns], preferred_element_type=F32)
            return weights[:, :128] + weights[:, 128:], product

        def add(parts, fresh):
            partial, product = parts[0]
            for more_partial, more_product in parts[1:]:
                partial = partial + more_partial
                product = product + more_product
            if fresh:
                den[u] = partial
                acc[u] = product
            else:
                den[u] += partial
                acc[u] += product

        def causal():
            return block(0, (key_row <= query_row) if tile == phase else None)

        def edge():
            return block(8, (key_row > query_row) if tile == phase else None)

        has_causal = phase <= tile
        has_edge = phase >= tile

        @pl.when(s >= 8)
        def _():
            parts = [block(slot, None) for slot in range(1, 8)]
            if has_causal:
                parts.insert(0, causal())
            if has_edge:
                parts.append(edge())
            add(parts, phase == 0)

        @pl.when(s < 8)
        def _():
            if phase == 0:
                add([causal()], True)
            elif has_causal:
                add([causal()], False)

            def single(j, carry):
                add([block(1 + j, None)], False)
                return carry

            lax.fori_loop(0, jnp.minimum(7, s), single, 0)

    lag = 1 + ((z == 1) & (x == 0)).astype(jnp.int32)
    first_attend = lag + 5

    def relayed(t, hops):
        return jnp.where(t >= CHUNKS + hops, CHUNKS, jnp.clip(t - lag + 1 - hops, 0, CHUNKS))

    def relay(t, hops, action):
        def one(i, carry):
            action(i)
            return carry

        lax.fori_loop(relayed(t - 1, hops), relayed(t, hops), one, 0)

    def step(t, carry):
        when(t < CHUNKS, lambda: own(t))
        when((t >= 1) & (t < CHUNKS + 1), lambda: relay_onward(t - 1))
        relay(t, 0, relay_far)
        relay(t, 1, relay_near)
        relay(t, 2, relay_second)

        @pl.when(t == 0)
        def _():
            for k in range(3):
                weight_along_y(k).wait_recv()
            weight_along_x(0).start()
            loads[3].wait()

        @pl.when(t == CHUNKS)
        def _():
            weight_along_x(0).wait_recv()
            weight_along_x(1).start()
            weight_along_x(2).start()

        when(t == 3, lambda: queries(0))
        when(t == CHUNKS - 1, lambda: queries(1))
        when(t == first_attend, lambda: sibling_arrivals(0, CHUNKS // 2))
        when((t >= first_attend) & (t < first_attend + 2), lambda: attend(t - first_attend, 0, 0))
        when((t >= first_attend + 2) & (t < first_attend + 4), lambda: attend(t - first_attend - 2, 1, 0))
        return carry

    lax.fori_loop(0, CHUNKS + 3, step, 0)
    sibling_arrivals(CHUNKS // 2, CHUNKS)
    loads[4].wait()

    def unit_exchange(u):
        return remote(att.at[head, u], att.at[head, u], att_send.at[u], att_recv.at[u], partner)

    def unit_arrival(u):
        return remote(att.at[head, u], att.at[other, u], att_send.at[u], att_recv.at[u], partner)

    def project(tile, which, groups, fresh):
        rows = slice(tile * TILE, (tile + 1) * TILE)

        def columns_of(j, carry):
            columns = aligned(j * 896, 896)
            product = None
            for group in groups:
                term = jnp.dot(
                    att[which, 2 * tile + group], wob[aligned(which * 1024 + group * 512, 512), columns],
                    preferred_element_type=F32,
                )
                product = term if product is None else product + term
            if fresh:
                branch[rows, columns] = product
            else:
                branch[rows, columns] += product
            return carry

        lax.fori_loop(0, HALF // 896, columns_of, 0)

    for tile in range(2):
        def second_phase(group, carry):
            u = 2 * tile + group
            attend(group, tile, 1)
            denominator = jnp.sum(den[u], axis=-1, keepdims=True)
            attended = (acc[u] / denominator).astype(BF16)
            att[head, u] = jnp.concatenate([attended[:TILE], attended[TILE:]], axis=1)
            unit_exchange(u).start()
            return carry

        lax.fori_loop(0, 2, second_phase, 0)
        if tile == 1:
            for hop in (1, 2):
                weight_along_x(hop).wait_recv()
            weight_sibling().start()
            for part in range(2):
                project(part, head, (0, 1), True)

    diagonal = lax.broadcasted_iota(jnp.int32, (128, 128), 0) == lax.broadcasted_iota(jnp.int32, (128, 128), 1)

    def sums_copy(tile):
        return remote(sums.at[0, tile], sums.at[1, tile], sum_send.at[tile], sum_recv.at[tile], partner)

    def send_sums(tile):
        share = branch[aligned(tile * TILE, TILE)]
        totals = jnp.sum(share * share, axis=-1, keepdims=True)
        for block in range(2):
            spread = jnp.where(diagonal, totals[block * 128 : (block + 1) * 128], 0.0)
            sums[0, tile, block * 8 : (block + 1) * 8] = jnp.broadcast_to(jnp.sum(spread, axis=0, keepdims=True), (8, 128))
        sums_copy(tile).start()

    def output_copy(tile):
        rows = aligned(tile * TILE, TILE)
        return pltpu.make_async_copy(obuf.at[rows], out.at[rows], out_sem.at[tile])

    def finish(tile):
        sums_copy(tile).wait_recv()
        for block in range(2):
            rows = aligned(tile * TILE + block * 128, 128)
            both = sums[0, tile, block * 8 : block * 8 + 1] + sums[1, tile, block * 8 : block * 8 + 1]
            squares = jnp.sum(jnp.where(diagonal, both, 0.0), axis=1, keepdims=True)
            inverse = lax.rsqrt(squares / D + norm_epsilon)
            obuf[rows] = (xbuf[head, rows].astype(F32) + post[...][None, :] * branch[rows] * inverse).astype(BF16)
        output_copy(tile).start()

    weight_sibling().wait_recv()
    unit_arrival(0).wait_recv()
    unit_arrival(1).wait_recv()
    project(0, other, (0, 1), False)
    send_sums(0)
    unit_arrival(2).wait_recv()
    project(1, other, (0,), False)
    unit_arrival(3).wait_recv()
    project(1, other, (1,), False)
    send_sums(1)
    finish(0)
    finish(1)

    def drain(i, carry):
        token_copy(i).wait_send()
        when(far_direct(i), lambda: far(i).wait_send())
        when(far_by_transit(i), lambda: far_transit(i).wait_send())
        when(onward_here(i), lambda: onward(i).wait_send())
        when(up_own | up_relay, lambda: up(i).wait_send())
        when(down_own | down_relay, lambda: down(i).wait_send())
        when(second_up_valid, lambda: second_up(i).wait_send())
        when(second_down_valid, lambda: second_down(i).wait_send())
        for slot in (0, 2, 4, 6, 8):
            sends = (slot <= s) & ((core == 0) if slot == 0 else (core == 1) if slot == 8 else (core >= 0))
            when(sends, lambda: to_sibling(i, slot).wait_send())
        return carry

    lax.fori_loop(0, CHUNKS, drain, 0)
    weight_slice().wait_send()
    for k in range(3):
        weight_along_y(k).wait_send()
        weight_along_x(k).wait_send()
    weight_sibling().wait_send()
    for u in range(UNITS):
        unit_exchange(u).wait_send()
    for tile in range(2):
        sums_copy(tile).wait_send()
        output_copy(tile).wait()


def local(tokens, pre_gain, query_weight, key_weight, value_weight, out_weight, post_gain):
    turns, frequency = rope_rows()
    vmem = pl.BlockSpec(memory_space=pltpu.VMEM)
    hbm = pl.BlockSpec(memory_space=pl.ANY)
    dma = pltpu.SemaphoreType.DMA
    return pl.pallas_call(
        layer_kernel,
        out_shape=jax.ShapeDtypeStruct((ROWS, HALF), BF16),
        in_specs=[hbm, vmem, hbm, hbm, hbm, hbm, vmem, vmem, vmem],
        out_specs=hbm,
        scratch_shapes=[
            pltpu.VMEM((2, ROWS, HALF), BF16),
            pltpu.VMEM((ROWS, D), BF16),
            pltpu.VMEM((D, 4 * HD), BF16),
            pltpu.VMEM((D, 2 * HD), BF16),
            pltpu.VMEM((D, 2 * HD), BF16),
            pltpu.VMEM((2048, HALF), BF16),
            pltpu.VMEM((4, ROWS, HD), BF16),
            pltpu.VMEM((SLOTS * ROWS, 4 * HD), BF16),
            pltpu.VMEM((UNITS, 2 * TILE, HD), F32),
            pltpu.VMEM((UNITS, 2 * TILE, 128), F32),
            pltpu.VMEM((2, UNITS, TILE, 2 * HD), BF16),
            pltpu.VMEM((ROWS, HALF), F32),
            pltpu.VMEM((3, PART, 4 * HD), BF16),
            pltpu.VMEM((2, 2, 16, 128), F32),
            pltpu.VMEM((ROWS, HALF), BF16),
            pltpu.VMEM((ROWS, HD // 2), F32),
            pltpu.VMEM((ROWS, HD // 2), F32),
            dma((5,)),
            dma((CHUNKS,)),
            dma((CHUNKS,)),
            dma((5, CHUNKS)),
            dma((4, CHUNKS)),
            dma((4, CHUNKS)),
            dma((4, CHUNKS)),
            dma((CHUNKS,)),
            dma((3,)),
            dma((3,)),
            dma((8,)),
            dma((8,)),
            dma((UNITS,)),
            dma((UNITS,)),
            dma((2,)),
            dma((2,)),
            dma((2,)),
        ],
        compiler_params=pltpu.CompilerParams(
            collective_id=0, has_side_effects=True, vmem_limit_bytes=63 * 1024 * 1024
        ),
        name="layer",
    )(
        tokens, pre_gain, query_weight, key_weight, value_weight, out_weight,
        post_gain, turns, frequency,
    )


def solution(mesh):
    placed = (
        P("seq", "head"),
        P(),
        P(None, "head"),
        P(None, "head"),
        P(None, "head"),
        P("head", None),
        P("head"),
    )
    return jax.shard_map(
        local, mesh=mesh, in_specs=placed, out_specs=P("seq", "head"), check_vma=False
    )
```

```python
import math

import jax
import jax.numpy as jnp
import numpy as np
from jax import lax
from jax.experimental import pallas as pl
from jax.experimental.pallas import tpu as pltpu
from jax.sharding import PartitionSpec as P

D = 3584
HALF = 1792
HD = 256
ROWS = 512
PART = 64
LONG = 7
CHUNKS = 9
HALF_READY = 4
SLOTS = 9
TILE = 256
UNITS = 4
MESH = pl.DeviceIdType.MESH
F32 = jnp.float32
BF16 = jnp.bfloat16
softcap_limit = 50.0
rope_base = 10000.0
norm_epsilon = 1e-06
EXP_SCALE = softcap_limit * math.log2(math.e)
SCORE_SCALE = HD ** (-0.5) / softcap_limit


def rope_rows():
    frequency = rope_base ** (-2.0 * np.arange(HD // 2) / HD)
    angles = np.arange(ROWS)[:, None] * frequency[None, :]
    table = np.stack([np.cos(angles), np.sin(angles)])
    return table.astype(np.float32), np.broadcast_to(frequency, (8, HD // 2)).astype(np.float32)


def aligned(start, size, step=None):
    return pl.ds(pl.multiple_of(start, step or size), size)


def chunk_rows(chunk, offset=0):
    index, size = chunk
    start = index * PART if size == PART else LONG * PART + (index - LONG) * size
    return aligned(offset + start, size)


def slot_rows(slot, chunk):
    return chunk_rows(chunk, (SLOTS - 1 - slot) * ROWS)


def each_chunk(first, last, action):
    def over(low, high, size):
        def one(i, carry):
            action((i, size))
            return carry

        lax.fori_loop(low, high, one, 0)

    over(first, jnp.minimum(last, LONG), PART)
    over(jnp.maximum(first, LONG), last, PART // 2)


def when(condition, action):
    pl.when(condition)(action)


def layer_kernel(
    tok, gain, wq, wk, wv, wo, post, turns, frequency, out,
    xbuf, xn, wqb, wkb, wvb, wob, q, kv, acc, den, att, branch, transit, sums, obuf, cosine, sine,
    load_sem, z_send, z_recv, send, recv, pair_send, pair_recv,
    transit_send, transit_recv, onward_send, across_send, w_send, w_recv, att_send, att_recv, sum_send, sum_recv, out_sem,
):
    s = lax.axis_index("seq")
    head = lax.axis_index("head")
    core = lax.rem(s, 2)
    chip = lax.div(s, 2)
    y = lax.rem(chip, 4)
    x = lax.rem(lax.div(chip, 4), 4)
    z = lax.div(chip, 16)
    other = 1 - head
    seq_up = s + jnp.where(y < 3, 2, -6)
    seq_down = s + jnp.where(y > 0, -2, 6)
    sibling = s + 1 - 2 * core
    has_next = chip < 28
    has_prev = chip >= 4
    crosses = (z == 0) & (x == 3)
    ring_y = [s + 2 * (lax.rem(y + k, 4) - y) for k in (1, 2, 3)]
    ring_x = [s + 8 * (lax.rem(x + k, 4) - x) for k in (1, 2, 3)]

    def at_seq(target):
        return (target, head)

    partner = (s, other)
    weight_partner = (s + 32 - 64 * z, other)

    def remote(source, target, send_sem, recv_sem, device):
        return pltpu.make_async_remote_copy(
            src_ref=source, dst_ref=target, send_sem=send_sem, recv_sem=recv_sem,
            device_id=device, device_id_type=MESH,
        )

    own_columns = aligned(head * HALF, HALF, 128)
    other_columns = aligned(other * HALF, HALF, 128)
    loads = [
        pltpu.make_async_copy(tok, xbuf.at[head], load_sem.at[0]),
        pltpu.make_async_copy(wv, wvb, load_sem.at[1]),
        pltpu.make_async_copy(wk, wkb, load_sem.at[2]),
        pltpu.make_async_copy(wq, wqb, load_sem.at[3]),
        pltpu.make_async_copy(wo.at[:, own_columns], wob.at[aligned(head * 1024, 1024)], load_sem.at[4]),
    ]
    for load in loads:
        load.start()

    barrier = pltpu.get_barrier_semaphore()

    def greet(device):
        pl.semaphore_signal(barrier, inc=1, device_id=device, device_id_type=MESH)

    greet(partner)
    greet(weight_partner)
    greet(at_seq(sibling))
    for target in ring_y + ring_x:
        greet(at_seq(target))

    @pl.when(z == 1)
    def _():
        greet(at_seq((12 + y) * 2 + core))

    @pl.when(crosses)
    def _():
        for column in range(4):
            greet(at_seq((16 + 4 * column + y) * 2 + core))

    crossing_pair = (crosses & (y >= 2)) | ((z == 1) & (x == 0) & (y < 2))

    @pl.when(crossing_pair)
    def _():
        greet(at_seq((14 + y) * 2 + core))

    pl.semaphore_wait(barrier, 9 + z + 4 * crosses.astype(jnp.int32) + crossing_pair.astype(jnp.int32))

    slice_index = (core * 4 + x) * 4 + y
    mine = head * 1024
    theirs = other * 1024

    def weight_slice():
        return remote(
            wo.at[aligned(slice_index * 32, 32), other_columns], wob.at[aligned(mine + slice_index * 32, 32)],
            w_send.at[0], w_recv.at[0], weight_partner,
        )

    def weight_along_y(k):
        rows = aligned(theirs + slice_index * 32, 32)
        return remote(wob.at[rows], wob.at[rows], w_send.at[1 + k], w_recv.at[1 + k], at_seq(ring_y[k]))

    def weight_along_x(hop):
        column = lax.rem(x + 1, 4) if hop == 1 else x
        rows = aligned(theirs + (core * 4 + column) * 128, 128)
        return remote(wob.at[rows], wob.at[rows], w_send.at[4 + hop], w_recv.at[4 + hop], at_seq(ring_x[0 if hop == 2 else 2]))

    def weight_sibling():
        rows = aligned(theirs + core * 512, 512)
        return remote(wob.at[rows], wob.at[rows], w_send.at[7], w_recv.at[7], at_seq(sibling))

    def token_copy(c):
        rows = chunk_rows(c)
        return remote(tok.at[rows], xbuf.at[head, rows], z_send.at[c[0]], z_recv.at[c[0]], partner)

    def token_arrival(c):
        rows = chunk_rows(c)
        return remote(tok.at[rows], xbuf.at[other, rows], z_send.at[c[0]], z_recv.at[c[0]], partner)

    def flow(index, c, source, slot, target):
        return remote(
            kv.at[slot_rows(source, c)], kv.at[slot_rows(slot, c)], send.at[index, c[0]], recv.at[index, c[0]],
            at_seq(target),
        )

    def far(c):
        return flow(0, c, 0, 8, s + 8)

    def transit_slot(c):
        return transit.at[lax.div(c[0], 3), pl.ds(0, c[1])]

    def far_transit(c):
        column = column_of(c)
        return remote(
            kv.at[slot_rows(0, c)], transit_slot(c), transit_send.at[c[0]], transit_recv.at[lax.div(c[0], 3)],
            at_seq((16 + 4 * column + y) * 2 + core),
        )

    def onward(c):
        return remote(
            transit_slot(c), kv.at[slot_rows(8, c)], onward_send.at[lax.div(c[0], 3)], recv.at[0, c[0]], at_seq(s - 8 * x)
        )

    def column_of(c):
        return jnp.where(c[0] < LONG - 1, lax.rem(c[0], 3), jnp.where(c[0] == LONG - 1, 1, 0))

    def in_own_column(c):
        return column_of(c) == 0

    def far_direct(c):
        return has_next & ((z == 1) | (x < 3) | in_own_column(c))

    def far_by_transit(c):
        return crosses & jnp.logical_not(in_own_column(c))

    def onward_here(c):
        return (z == 1) & (x > 0) & (column_of(c) == x)

    def across(c):
        return remote(
            kv.at[slot_rows(0, c)], kv.at[slot_rows(4, c)], across_send.at[c[0] - LONG], recv.at[3, c[0]],
            at_seq((14 + y) * 2 + core),
        )

    def up(c):
        return flow(1, c, jnp.where(y < 3, 0, 8), 2, seq_up)

    def down(c):
        return flow(2, c, jnp.where(y == 0, 0, 8), 6, seq_down)

    def second_up(c):
        return flow(3, c, 2, 4, seq_up)

    def second_down(c):
        return remote(
            kv.at[slot_rows(6, c)], kv.at[slot_rows(4, c)], send.at[4, c[0]], recv.at[3, c[0]], at_seq(seq_down)
        )

    def to_sibling(c, slot):
        target = slot + 1 - 2 * core
        lane = lax.div(target - 1, 2)
        return remote(
            kv.at[slot_rows(slot, c)], kv.at[slot_rows(target, c)], pair_send.at[lane, c[0]], pair_recv.at[lane, c[0]],
            at_seq(sibling),
        )

    up_own = y < 3
    up_relay = (y == 3) & has_prev
    down_own = y == 0
    down_relay = (y > 0) & has_prev
    crossed = (z == 1) & (x == 0)
    goes_across = crosses & (y >= 2)

    def second_up_valid(c):
        valid = (y < 3) & (chip >= 1)
        return valid if c[1] == PART else valid & jnp.logical_not(crossed & (y == 0))

    def second_down_valid(c):
        valid = (y == 1) & has_prev
        return valid if c[1] == PART else valid & jnp.logical_not(crossed)


    weight_slice().start()
    each_chunk(0, CHUNKS, lambda c: token_copy(c).start())
    base = jnp.sum(jnp.where(lax.broadcasted_iota(jnp.int32, (8, HD // 2), 0) == 0, frequency[...], 0.0), axis=0, keepdims=True)
    base = base * (s * ROWS).astype(F32)
    base_cos = jnp.cos(base)
    base_sin = jnp.sin(base)
    cosine[...] = base_cos * turns[0] - base_sin * turns[1]
    sine[...] = base_sin * turns[0] + base_cos * turns[1]
    for load in loads[:3]:
        load.wait()
    weight_slice().wait_recv()
    for k in range(3):
        weight_along_y(k).start()

    def roped(values, rows):
        cos = cosine[rows]
        sin = sine[rows]
        leading = values[:, : HD // 2]
        trailing = values[:, HD // 2 :]
        return jnp.concatenate([leading * cos - trailing * sin, trailing * cos + leading * sin], axis=1).astype(BF16)

    def own(c):
        token_arrival(c).wait_recv()
        rows = chunk_rows(c)
        first = xbuf[0, rows].astype(F32)
        second = xbuf[1, rows].astype(F32)
        squares = jnp.sum(first * first, axis=-1, keepdims=True) + jnp.sum(second * second, axis=-1, keepdims=True)
        scale = lax.rsqrt(squares / D + norm_epsilon)
        xn[rows, :HALF] = (first * scale * gain[:HALF][None, :]).astype(BF16)
        xn[rows, HALF:] = (second * scale * gain[HALF:][None, :]).astype(BF16)

        def value(j, carry):
            product = jnp.dot(xn[rows], wvb[:, aligned(j * HD, HD)], preferred_element_type=F32)
            kv[slot_rows(0, c), aligned(2 * HD + j * HD, HD)] = product.astype(BF16)
            return carry

        def key(j, carry):
            columns = aligned(j * HD, HD)
            product = jnp.dot(xn[rows], wkb[:, columns], preferred_element_type=F32)
            kv[slot_rows(0, c), columns] = roped(product, rows)
            return carry

        lax.fori_loop(0, 2, value, 0)
        lax.fori_loop(0, 2, key, 0)
        when(far_direct(c), lambda: far(c).start())
        when(far_by_transit(c), lambda: far_transit(c).start())
        if c[1] < PART:
            when(goes_across, lambda: across(c).start())
        when(up_own, lambda: up(c).start())
        when(down_own, lambda: down(c).start())
        when(core == 0, lambda: to_sibling(c, 0).start())

    def queries(tile):
        rows = aligned(tile * TILE, TILE)

        def query(j, carry):
            product = jnp.dot(xn[rows], wqb[:, aligned(j * HD, HD)], preferred_element_type=F32)
            q[j, rows] = roped(product, rows)
            return carry

        lax.fori_loop(0, 4, query, 0)

    def relay_onward(c):
        @pl.when(onward_here(c))
        def _():
            far_transit(c).wait_recv()
            onward(c).start()

    def relay_far(c):
        @pl.when(has_prev)
        def _():
            far(c).wait_recv()
            when(up_relay, lambda: up(c).start())
            when(down_relay, lambda: down(c).start())
            when(core == 1, lambda: to_sibling(c, 8).start())

    def relay_up(c):
        @pl.when(chip >= 1)
        def _():
            up(c).wait_recv()
            when(second_up_valid(c), lambda: second_up(c).start())
            to_sibling(c, 2).start()

    def relay_down(c):
        @pl.when(chip >= 3)
        def _():
            down(c).wait_recv()
            when(second_down_valid(c), lambda: second_down(c).start())
            to_sibling(c, 6).start()

    def relay_second(c):
        @pl.when(chip >= 2)
        def _():
            second_up(c).wait_recv()
            to_sibling(c, 4).start()

    def sibling_arrivals(first, last):
        def arrivals(c):
            for lane in range(4):
                @pl.when(s >= 2 * lane + 1)
                def _():
                    rows = slot_rows(2 * lane + 1, c)
                    remote(
                        kv.at[rows], kv.at[rows], pair_send.at[lane, c[0]], pair_recv.at[lane, c[0]], at_seq(sibling)
                    ).wait_recv()

        each_chunk(first, last, arrivals)

    query_row = lax.rem(lax.broadcasted_iota(jnp.int32, (2 * TILE, TILE), 0), TILE)
    key_row = lax.broadcasted_iota(jnp.int32, (2 * TILE, TILE), 1)

    def attend(group, tile, phase):
        u = 2 * tile + group
        key_columns = aligned(group * HD, HD)
        value_columns = aligned(2 * HD + group * HD, HD)
        query = q[pl.ds(2 * group, 2), tile * TILE : (tile + 1) * TILE].reshape(2 * TILE, HD)

        def block(slot, mask):
            rows = aligned((SLOTS - 1 - slot) * ROWS + phase * TILE, TILE)
            scores = lax.dot_general(
                query, kv[rows, key_columns], (((1,), (1,)), ((), ())), preferred_element_type=F32
            )
            weights = jnp.exp2(EXP_SCALE * jnp.tanh(scores * SCORE_SCALE))
            if mask is not None:
                weights = jnp.where(mask, weights, 0.0)
            product = jnp.dot(weights.astype(BF16), kv[rows, value_columns], preferred_element_type=F32)
            return weights[:, :128] + weights[:, 128:], product

        def add(parts, fresh):
            partial, product = parts[0]
            for more_partial, more_product in parts[1:]:
                partial = partial + more_partial
                product = product + more_product
            if fresh:
                den[u] = partial
                acc[u] = product
            else:
                den[u] += partial
                acc[u] += product

        def causal():
            return block(0, (key_row <= query_row) if tile == phase else None)

        def edge():
            return block(8, (key_row > query_row) if tile == phase else None)

        has_causal = phase <= tile
        has_edge = phase >= tile

        @pl.when(s >= 8)
        def _():
            parts = [block(slot, None) for slot in range(1, 8)]
            if has_causal:
                parts.insert(0, causal())
            if has_edge:
                parts.append(edge())
            add(parts, phase == 0)

        @pl.when(s < 8)
        def _():
            if phase == 0:
                add([causal()], True)
            elif has_causal:
                add([causal()], False)

            def single(j, carry):
                add([block(1 + j, None)], False)
                return carry

            lax.fori_loop(0, jnp.minimum(7, s), single, 0)

    late = crossed | crosses
    far_lag = jnp.where(crossed, 2, 1)
    near_lag = jnp.where(far_lag == 1, 2, far_lag + 1)
    up_lag = jnp.where(y == 0, near_lag, 2)
    down_lag = jnp.where(y == 3, 2, near_lag)
    second_lag = jnp.where(y < 2, near_lag + 2, 4)
    half_step = jnp.where(late, CHUNKS + 1, jnp.maximum(jnp.maximum(up_lag, down_lag), second_lag) + HALF_READY - 1)
    half_units = jnp.where(late, 1, 2)

    def relayed(t, lag, hops):
        return jnp.where(
            t >= CHUNKS + hops // 2, jnp.minimum(t - hops, CHUNKS), jnp.clip(t + 1 - lag, 0, CHUNKS)
        )

    def relay(t, lag, hops, action):
        each_chunk(relayed(t - 1, lag, hops), relayed(t, lag, hops), action)

    def step(t, carry):
        each_chunk(t, jnp.minimum(t + 1, CHUNKS), own)
        each_chunk(jnp.maximum(t - 1, 0), jnp.minimum(t, CHUNKS), relay_onward)
        relay(t, far_lag, 0, relay_far)
        relay(t, up_lag, 1, relay_up)
        relay(t, down_lag, 1, relay_down)
        relay(t, second_lag, 2, relay_second)

        @pl.when(t == 1)
        def _():
            for k in range(3):
                weight_along_y(k).wait_recv()
            weight_along_x(0).start()

        when(t == 0, lambda: loads[3].wait())

        @pl.when(t == CHUNKS)
        def _():
            weight_along_x(0).wait_recv()
            weight_along_x(1).start()
            weight_along_x(2).start()

        when(t == 3, lambda: queries(0))
        when(t == half_step, lambda: sibling_arrivals(0, HALF_READY))
        when((t >= half_step) & (t < half_step + half_units), lambda: attend(t - half_step, 0, 0))
        when(t == 9, lambda: queries(1))
        when((t == CHUNKS + 1) & jnp.logical_not(late), lambda: attend(0, 1, 0))
        return carry

    lax.fori_loop(0, CHUNKS + 3, step, 0)
    sibling_arrivals(HALF_READY, CHUNKS)
    loads[4].wait()

    def unit_exchange(u):
        return remote(att.at[head, u], att.at[head, u], att_send.at[u], att_recv.at[u], partner)

    def unit_arrival(u):
        return remote(att.at[head, u], att.at[other, u], att_send.at[u], att_recv.at[u], partner)

    def project(tile, which, groups, fresh):
        rows = slice(tile * TILE, (tile + 1) * TILE)

        def columns_of(j, carry):
            columns = aligned(j * 896, 896)
            product = None
            for group in groups:
                term = jnp.dot(
                    att[which, 2 * tile + group], wob[aligned(which * 1024 + group * 512, 512), columns],
                    preferred_element_type=F32,
                )
                product = term if product is None else product + term
            if fresh:
                branch[rows, columns] = product
            else:
                branch[rows, columns] += product
            return carry

        lax.fori_loop(0, HALF // 896, columns_of, 0)

    for tile in range(2):
        def second_phase(group, carry):
            u = 2 * tile + group
            if tile == 0:
                when(late & (group == 1), lambda: attend(1, 0, 0))
            attend(group, tile, 1)
            denominator = jnp.sum(den[u], axis=-1, keepdims=True)
            attended = (acc[u] / denominator).astype(BF16)
            att[head, u] = jnp.concatenate([attended[:TILE], attended[TILE:]], axis=1)
            unit_exchange(u).start()
            return carry

        lax.fori_loop(0, 2, second_phase, 0)
        if tile == 0:
            when(late, lambda: attend(0, 1, 0))
            attend(1, 1, 0)
        else:
            project(0, head, (0, 1), True)
            for hop in (1, 2):
                weight_along_x(hop).wait_recv()
            weight_sibling().start()
            project(1, head, (0, 1), True)

    diagonal = lax.broadcasted_iota(jnp.int32, (128, 128), 0) == lax.broadcasted_iota(jnp.int32, (128, 128), 1)

    def sums_copy(tile):
        return remote(sums.at[0, tile], sums.at[1, tile], sum_send.at[tile], sum_recv.at[tile], partner)

    def send_sums(tile):
        share = branch[aligned(tile * TILE, TILE)]
        totals = jnp.sum(share * share, axis=-1, keepdims=True)
        for block in range(2):
            spread = jnp.where(diagonal, totals[block * 128 : (block + 1) * 128], 0.0)
            sums[0, tile, block * 8 : (block + 1) * 8] = jnp.broadcast_to(jnp.sum(spread, axis=0, keepdims=True), (8, 128))
        sums_copy(tile).start()

    def output_copy(tile):
        rows = aligned(tile * TILE, TILE)
        return pltpu.make_async_copy(obuf.at[rows], out.at[rows], out_sem.at[tile])

    def finish(tile):
        sums_copy(tile).wait_recv()
        for block in range(2):
            rows = aligned(tile * TILE + block * 128, 128)
            both = sums[0, tile, block * 8 : block * 8 + 1] + sums[1, tile, block * 8 : block * 8 + 1]
            squares = jnp.sum(jnp.where(diagonal, both, 0.0), axis=1, keepdims=True)
            inverse = lax.rsqrt(squares / D + norm_epsilon)
            obuf[rows] = (xbuf[head, rows].astype(F32) + post[...][None, :] * branch[rows] * inverse).astype(BF16)
        output_copy(tile).start()

    def drain(c):
        token_copy(c).wait_send()
        when(far_direct(c), lambda: far(c).wait_send())
        when(far_by_transit(c), lambda: far_transit(c).wait_send())
        when(onward_here(c), lambda: onward(c).wait_send())
        if c[1] < PART:
            when(goes_across, lambda: across(c).wait_send())
        when(up_own | up_relay, lambda: up(c).wait_send())
        when(down_own | down_relay, lambda: down(c).wait_send())
        when(second_up_valid(c), lambda: second_up(c).wait_send())
        when(second_down_valid(c), lambda: second_down(c).wait_send())
        for slot in (0, 2, 4, 6, 8):
            sends = (slot <= s) & ((core == 0) if slot == 0 else (core == 1) if slot == 8 else (core >= 0))
            when(sends, lambda: to_sibling(c, slot).wait_send())

    weight_sibling().wait_recv()
    unit_arrival(0).wait_recv()
    unit_arrival(1).wait_recv()
    project(0, other, (0, 1), False)
    send_sums(0)
    unit_arrival(2).wait_recv()
    project(1, other, (0,), False)
    each_chunk(0, CHUNKS, drain)
    weight_slice().wait_send()
    for k in range(3):
        weight_along_y(k).wait_send()
        weight_along_x(k).wait_send()
    weight_sibling().wait_send()
    unit_arrival(3).wait_recv()
    project(1, other, (1,), False)
    send_sums(1)
    finish(0)
    finish(1)

    for u in range(UNITS):
        unit_exchange(u).wait_send()
    for tile in range(2):
        sums_copy(tile).wait_send()
        output_copy(tile).wait()


def local(tokens, pre_gain, query_weight, key_weight, value_weight, out_weight, post_gain):
    turns, frequency = rope_rows()
    vmem = pl.BlockSpec(memory_space=pltpu.VMEM)
    hbm = pl.BlockSpec(memory_space=pl.ANY)
    dma = pltpu.SemaphoreType.DMA
    return pl.pallas_call(
        layer_kernel,
        out_shape=jax.ShapeDtypeStruct((ROWS, HALF), BF16),
        in_specs=[hbm, vmem, hbm, hbm, hbm, hbm, vmem, vmem, vmem],
        out_specs=hbm,
        scratch_shapes=[
            pltpu.VMEM((2, ROWS, HALF), BF16),
            pltpu.VMEM((ROWS, D), BF16),
            pltpu.VMEM((D, 4 * HD), BF16),
            pltpu.VMEM((D, 2 * HD), BF16),
            pltpu.VMEM((D, 2 * HD), BF16),
            pltpu.VMEM((2048, HALF), BF16),
            pltpu.VMEM((4, ROWS, HD), BF16),
            pltpu.VMEM((SLOTS * ROWS, 4 * HD), BF16),
            pltpu.VMEM((UNITS, 2 * TILE, HD), F32),
            pltpu.VMEM((UNITS, 2 * TILE, 128), F32),
            pltpu.VMEM((2, UNITS, TILE, 2 * HD), BF16),
            pltpu.VMEM((ROWS, HALF), F32),
            pltpu.VMEM((3, PART, 4 * HD), BF16),
            pltpu.VMEM((2, 2, 16, 128), F32),
            pltpu.VMEM((ROWS, HALF), BF16),
            pltpu.VMEM((ROWS, HD // 2), F32),
            pltpu.VMEM((ROWS, HD // 2), F32),
            dma((5,)),
            dma((CHUNKS,)),
            dma((CHUNKS,)),
            dma((5, CHUNKS)),
            dma((4, CHUNKS)),
            dma((4, CHUNKS)),
            dma((4, CHUNKS)),
            dma((CHUNKS,)),
            dma((3,)),
            dma((3,)),
            dma((2,)),
            dma((8,)),
            dma((8,)),
            dma((UNITS,)),
            dma((UNITS,)),
            dma((2,)),
            dma((2,)),
            dma((2,)),
        ],
        compiler_params=pltpu.CompilerParams(
            collective_id=0, has_side_effects=True, vmem_limit_bytes=63 * 1024 * 1024
        ),
        name="layer",
    )(
        tokens, pre_gain, query_weight, key_weight, value_weight, out_weight,
        post_gain, turns, frequency,
    )


def solution(mesh):
    placed = (
        P("seq", "head"),
        P(),
        P(None, "head"),
        P(None, "head"),
        P(None, "head"),
        P("head", None),
        P("head"),
    )
    return jax.shard_map(
        local, mesh=mesh, in_specs=placed, out_specs=P("seq", "head"), check_vma=False
    )
```

```python
import math

import jax
import jax.numpy as jnp
import numpy as np
from jax import lax
from jax.experimental import pallas as pl
from jax.experimental.pallas import tpu as pltpu
from jax.sharding import PartitionSpec as P

D = 3584
HALF = 1792
HD = 256
ROWS = 512
PART = 64
LONG = 7
CHUNKS = 9
HALF_READY = 4
SLOTS = 9
TILE = 256
UNITS = 4
MESH = pl.DeviceIdType.MESH
F32 = jnp.float32
BF16 = jnp.bfloat16
softcap_limit = 50.0
rope_base = 10000.0
norm_epsilon = 1e-06
EXP_SCALE = softcap_limit * math.log2(math.e)
SCORE_SCALE = HD ** (-0.5) / softcap_limit


def rope_rows():
    frequency = rope_base ** (-2.0 * np.arange(HD // 2) / HD)
    angles = np.arange(ROWS)[:, None] * frequency[None, :]
    table = np.stack([np.cos(angles), np.sin(angles)])
    return table.astype(np.float32), np.broadcast_to(frequency, (8, HD // 2)).astype(np.float32)


def aligned(start, size, step=None):
    return pl.ds(pl.multiple_of(start, step or size), size)


def chunk_rows(chunk, offset=0):
    index, size = chunk
    start = index * PART if size == PART else LONG * PART + (index - LONG) * size
    return aligned(offset + start, size)


def slot_rows(slot, chunk):
    return chunk_rows(chunk, (SLOTS - 1 - slot) * ROWS)


def each_chunk(first, last, action):
    def over(low, high, size):
        def one(i, carry):
            action((i, size))
            return carry

        lax.fori_loop(low, high, one, 0)

    over(first, jnp.minimum(last, LONG), PART)
    over(jnp.maximum(first, LONG), last, PART // 2)


def when(condition, action):
    pl.when(condition)(action)


def layer_kernel(
    tok, gain, wq, wk, wv, wo, post, turns, frequency, out,
    xbuf, xn, wqb, wkb, wvb, wob, q, kv, acc, den, att, branch, transit, sums, obuf, cosine, sine,
    load_sem, z_send, z_recv, send, recv, pair_send, pair_recv,
    transit_send, transit_recv, onward_send, across_send, w_send, w_recv, att_send, att_recv, sum_send, sum_recv, out_sem,
):
    s = lax.axis_index("seq")
    head = lax.axis_index("head")
    core = lax.rem(s, 2)
    chip = lax.div(s, 2)
    y = lax.rem(chip, 4)
    x = lax.rem(lax.div(chip, 4), 4)
    z = lax.div(chip, 16)
    other = 1 - head
    seq_up = s + jnp.where(y < 3, 2, -6)
    seq_down = s + jnp.where(y > 0, -2, 6)
    sibling = s + 1 - 2 * core
    has_next = chip < 28
    has_prev = chip >= 4
    crosses = (z == 0) & (x == 3)
    ring_y = [s + 2 * (lax.rem(y + k, 4) - y) for k in (1, 2, 3)]
    ring_x = [s + 8 * (lax.rem(x + k, 4) - x) for k in (1, 2, 3)]

    def at_seq(target):
        return (target, head)

    partner = (s, other)
    weight_partner = (s + 32 - 64 * z, other)

    def remote(source, target, send_sem, recv_sem, device):
        return pltpu.make_async_remote_copy(
            src_ref=source, dst_ref=target, send_sem=send_sem, recv_sem=recv_sem,
            device_id=device, device_id_type=MESH,
        )

    own_columns = aligned(head * HALF, HALF, 128)
    other_columns = aligned(other * HALF, HALF, 128)
    loads = [
        pltpu.make_async_copy(tok, xbuf.at[head], load_sem.at[0]),
        pltpu.make_async_copy(wv, wvb, load_sem.at[1]),
        pltpu.make_async_copy(wk, wkb, load_sem.at[2]),
        pltpu.make_async_copy(wq, wqb, load_sem.at[3]),
        pltpu.make_async_copy(wo.at[:, own_columns], wob.at[aligned(head * 1024, 1024)], load_sem.at[4]),
    ]
    for load in loads:
        load.start()

    barrier = pltpu.get_barrier_semaphore()

    def greet(device):
        pl.semaphore_signal(barrier, inc=1, device_id=device, device_id_type=MESH)

    greet(partner)
    greet(weight_partner)
    greet(at_seq(sibling))
    for target in ring_y + ring_x:
        greet(at_seq(target))

    @pl.when(z == 1)
    def _():
        greet(at_seq((12 + y) * 2 + core))

    @pl.when(crosses)
    def _():
        for column in range(4):
            greet(at_seq((16 + 4 * column + y) * 2 + core))

    @pl.when(crosses & (y >= 1))
    def _():
        greet(at_seq(jnp.where(y == 1, 16, 14 + y) * 2 + core))

    @pl.when((z == 1) & (x == 0) & (y < 2))
    def _():
        greet(at_seq((14 + y) * 2 + core))

    @pl.when((z == 1) & (x == 0) & (y == 0))
    def _():
        greet(at_seq(13 * 2 + core))

    pairs_across = jnp.where(crosses, jnp.minimum(y, 1), jnp.where((z == 1) & (x == 0), jnp.maximum(2 - y, 0), 0))
    pl.semaphore_wait(barrier, 9 + z + 4 * crosses.astype(jnp.int32) + pairs_across)

    slice_index = (core * 4 + x) * 4 + y
    mine = head * 1024
    theirs = other * 1024

    def weight_slice():
        return remote(
            wo.at[aligned(slice_index * 32, 32), other_columns], wob.at[aligned(mine + slice_index * 32, 32)],
            w_send.at[0], w_recv.at[0], weight_partner,
        )

    def weight_along_y(k):
        rows = aligned(theirs + slice_index * 32, 32)
        return remote(wob.at[rows], wob.at[rows], w_send.at[1 + k], w_recv.at[1 + k], at_seq(ring_y[k]))

    def weight_along_x(hop):
        column = lax.rem(x + 1, 4) if hop == 1 else x
        rows = aligned(theirs + (core * 4 + column) * 128, 128)
        return remote(wob.at[rows], wob.at[rows], w_send.at[4 + hop], w_recv.at[4 + hop], at_seq(ring_x[0 if hop == 2 else 2]))

    def weight_sibling():
        rows = aligned(theirs + core * 512, 512)
        return remote(wob.at[rows], wob.at[rows], w_send.at[7], w_recv.at[7], at_seq(sibling))

    def token_copy(c):
        rows = chunk_rows(c)
        return remote(tok.at[rows], xbuf.at[head, rows], z_send.at[c[0]], z_recv.at[c[0]], partner)

    def token_arrival(c):
        rows = chunk_rows(c)
        return remote(tok.at[rows], xbuf.at[other, rows], z_send.at[c[0]], z_recv.at[c[0]], partner)

    def flow(index, c, source, slot, target):
        return remote(
            kv.at[slot_rows(source, c)], kv.at[slot_rows(slot, c)], send.at[index, c[0]], recv.at[index, c[0]],
            at_seq(target),
        )

    def far(c):
        return flow(0, c, 0, 8, s + 8)

    def transit_slot(c):
        return transit.at[lax.div(c[0], 3), pl.ds(0, c[1])]

    def far_transit(c):
        column = column_of(c)
        return remote(
            kv.at[slot_rows(0, c)], transit_slot(c), transit_send.at[c[0]], transit_recv.at[lax.div(c[0], 3)],
            at_seq((16 + 4 * column + y) * 2 + core),
        )

    def onward(c):
        return remote(
            transit_slot(c), kv.at[slot_rows(8, c)], onward_send.at[lax.div(c[0], 3)], recv.at[0, c[0]], at_seq(s - 8 * x)
        )

    def column_of(c):
        return jnp.where(c[0] < LONG - 1, lax.rem(c[0], 3), jnp.where(c[0] == LONG - 1, 1, 0))

    def in_own_column(c):
        return column_of(c) == 0

    def far_direct(c):
        return has_next & ((z == 1) | (x < 3) | in_own_column(c))

    def far_by_transit(c):
        return crosses & jnp.logical_not(in_own_column(c))

    def onward_here(c):
        return (z == 1) & (x > 0) & (column_of(c) == x)

    def across(c):
        return remote(
            kv.at[slot_rows(0, c)], kv.at[slot_rows(jnp.where(y == 1, 6, 4), c)], across_send.at[c[0] - LONG],
            recv.at[jnp.where(y == 1, 2, 3), c[0]], at_seq(across_target),
        )

    def up(c):
        return flow(1, c, jnp.where(y < 3, 0, 8), 2, seq_up)

    def down(c):
        return flow(2, c, jnp.where(y == 0, 0, 8), 6, seq_down)

    def second_up(c):
        return flow(3, c, 2, 4, seq_up)

    def second_down(c):
        return remote(
            kv.at[slot_rows(6, c)], kv.at[slot_rows(4, c)], send.at[4, c[0]], recv.at[3, c[0]], at_seq(seq_down)
        )

    def to_sibling(c, slot):
        target = slot + 1 - 2 * core
        lane = lax.div(target - 1, 2)
        return remote(
            kv.at[slot_rows(slot, c)], kv.at[slot_rows(target, c)], pair_send.at[lane, c[0]], pair_recv.at[lane, c[0]],
            at_seq(sibling),
        )

    up_own = y < 3
    up_relay = (y == 3) & has_prev
    down_own = y == 0
    crossed = (z == 1) & (x == 0)
    goes_across = crosses & (y >= 1)
    across_target = jnp.where(y == 1, 16, 14 + y) * 2 + core

    def down_valid(c):
        relays = (y > 0) & has_prev
        return down_own | (relays if c[1] == PART else relays & jnp.logical_not(crossed & (y == 1)))

    def second_up_valid(c):
        valid = (y < 3) & (chip >= 1)
        return valid if c[1] == PART else valid & jnp.logical_not(crossed & (y == 0))

    def second_down_valid(c):
        valid = (y == 1) & has_prev
        return valid if c[1] == PART else valid & jnp.logical_not(crossed)


    weight_slice().start()
    each_chunk(0, CHUNKS, lambda c: token_copy(c).start())
    base = jnp.sum(jnp.where(lax.broadcasted_iota(jnp.int32, (8, HD // 2), 0) == 0, frequency[...], 0.0), axis=0, keepdims=True)
    base = base * (s * ROWS).astype(F32)
    base_cos = jnp.cos(base)
    base_sin = jnp.sin(base)
    cosine[...] = base_cos * turns[0] - base_sin * turns[1]
    sine[...] = base_sin * turns[0] + base_cos * turns[1]
    for load in loads[:3]:
        load.wait()
    weight_slice().wait_recv()
    for k in range(3):
        weight_along_y(k).start()

    def roped(values, rows):
        cos = cosine[rows]
        sin = sine[rows]
        leading = values[:, : HD // 2]
        trailing = values[:, HD // 2 :]
        return jnp.concatenate([leading * cos - trailing * sin, trailing * cos + leading * sin], axis=1).astype(BF16)

    def own(c):
        token_arrival(c).wait_recv()
        rows = chunk_rows(c)
        first = xbuf[0, rows].astype(F32)
        second = xbuf[1, rows].astype(F32)
        squares = jnp.sum(first * first, axis=-1, keepdims=True) + jnp.sum(second * second, axis=-1, keepdims=True)
        scale = lax.rsqrt(squares / D + norm_epsilon)
        xn[rows, :HALF] = (first * scale * gain[:HALF][None, :]).astype(BF16)
        xn[rows, HALF:] = (second * scale * gain[HALF:][None, :]).astype(BF16)

        def value(j, carry):
            product = jnp.dot(xn[rows], wvb[:, aligned(j * HD, HD)], preferred_element_type=F32)
            kv[slot_rows(0, c), aligned(2 * HD + j * HD, HD)] = product.astype(BF16)
            return carry

        def key(j, carry):
            columns = aligned(j * HD, HD)
            product = jnp.dot(xn[rows], wkb[:, columns], preferred_element_type=F32)
            kv[slot_rows(0, c), columns] = roped(product, rows)
            return carry

        lax.fori_loop(0, 2, value, 0)
        lax.fori_loop(0, 2, key, 0)
        when(far_direct(c), lambda: far(c).start())
        when(far_by_transit(c), lambda: far_transit(c).start())
        if c[1] < PART:
            when(goes_across, lambda: across(c).start())
        when(up_own, lambda: up(c).start())
        when(down_own, lambda: down(c).start())
        when(core == 0, lambda: to_sibling(c, 0).start())

    def queries(tile):
        rows = aligned(tile * TILE, TILE)

        def query(j, carry):
            product = jnp.dot(xn[rows], wqb[:, aligned(j * HD, HD)], preferred_element_type=F32)
            q[j, rows] = roped(product, rows)
            return carry

        lax.fori_loop(0, 4, query, 0)

    def relay_onward(c):
        @pl.when(onward_here(c))
        def _():
            far_transit(c).wait_recv()
            onward(c).start()

    def relay_far(c):
        @pl.when(has_prev)
        def _():
            far(c).wait_recv()
            when(up_relay, lambda: up(c).start())
            when(down_valid(c) & (y > 0), lambda: down(c).start())
            when(core == 1, lambda: to_sibling(c, 8).start())

    def relay_up(c):
        @pl.when(chip >= 1)
        def _():
            up(c).wait_recv()
            when(second_up_valid(c), lambda: second_up(c).start())
            to_sibling(c, 2).start()

    def relay_down(c):
        @pl.when(chip >= 3)
        def _():
            down(c).wait_recv()
            when(second_down_valid(c), lambda: second_down(c).start())
            to_sibling(c, 6).start()

    def relay_second(c):
        @pl.when(chip >= 2)
        def _():
            second_up(c).wait_recv()
            to_sibling(c, 4).start()

    def sibling_arrivals(first, last):
        def arrivals(c):
            for lane in range(4):
                @pl.when(s >= 2 * lane + 1)
                def _():
                    rows = slot_rows(2 * lane + 1, c)
                    remote(
                        kv.at[rows], kv.at[rows], pair_send.at[lane, c[0]], pair_recv.at[lane, c[0]], at_seq(sibling)
                    ).wait_recv()

        each_chunk(first, last, arrivals)

    query_row = lax.rem(lax.broadcasted_iota(jnp.int32, (2 * TILE, TILE), 0), TILE)
    key_row = lax.broadcasted_iota(jnp.int32, (2 * TILE, TILE), 1)

    def attend(group, tile, phase):
        u = 2 * tile + group
        key_columns = aligned(group * HD, HD)
        value_columns = aligned(2 * HD + group * HD, HD)
        query = q[pl.ds(2 * group, 2), tile * TILE : (tile + 1) * TILE].reshape(2 * TILE, HD)

        def block(slot, mask):
            rows = aligned((SLOTS - 1 - slot) * ROWS + phase * TILE, TILE)
            scores = lax.dot_general(
                query, kv[rows, key_columns], (((1,), (1,)), ((), ())), preferred_element_type=F32
            )
            weights = jnp.exp2(EXP_SCALE * jnp.tanh(scores * SCORE_SCALE))
            if mask is not None:
                weights = jnp.where(mask, weights, 0.0)
            product = jnp.dot(weights.astype(BF16), kv[rows, value_columns], preferred_element_type=F32)
            return weights[:, :128] + weights[:, 128:], product

        def add(parts, fresh):
            partial, product = parts[0]
            for more_partial, more_product in parts[1:]:
                partial = partial + more_partial
                product = product + more_product
            if fresh:
                den[u] = partial
                acc[u] = product
            else:
                den[u] += partial
                acc[u] += product

        def causal():
            return block(0, (key_row <= query_row) if tile == phase else None)

        def edge():
            return block(8, (key_row > query_row) if tile == phase else None)

        has_causal = phase <= tile
        has_edge = phase >= tile

        @pl.when(s >= 8)
        def _():
            parts = [block(slot, None) for slot in range(1, 8)]
            if has_causal:
                parts.insert(0, causal())
            if has_edge:
                parts.append(edge())
            add(parts, phase == 0)

        @pl.when(s < 8)
        def _():
            if phase == 0:
                add([causal()], True)
            elif has_causal:
                add([causal()], False)

            def single(j, carry):
                add([block(1 + j, None)], False)
                return carry

            lax.fori_loop(0, jnp.minimum(7, s), single, 0)

    late = crossed | crosses
    far_lag = jnp.where(crossed, 2, 1)
    near_lag = jnp.where(far_lag == 1, 2, far_lag + 1)
    up_lag = jnp.where(y == 0, near_lag, 2)
    down_lag = jnp.where(y == 3, 2, near_lag)
    second_lag = jnp.where(y < 2, near_lag + 2, 4)
    half_step = jnp.where(late, CHUNKS + 1, jnp.maximum(jnp.maximum(up_lag, down_lag), second_lag) + HALF_READY - 1)
    half_units = jnp.where(late, 1, 2)

    def relayed(t, lag, hops):
        return jnp.where(
            t >= CHUNKS + hops // 2, jnp.minimum(t - hops, CHUNKS), jnp.clip(t + 1 - lag, 0, CHUNKS)
        )

    def relay(t, lag, hops, action):
        each_chunk(relayed(t - 1, lag, hops), relayed(t, lag, hops), action)

    def step(t, carry):
        each_chunk(t, jnp.minimum(t + 1, CHUNKS), own)
        each_chunk(jnp.maximum(t - 1, 0), jnp.minimum(t, CHUNKS), relay_onward)
        relay(t, far_lag, 0, relay_far)
        relay(t, up_lag, 1, relay_up)
        relay(t, down_lag, 1, relay_down)
        relay(t, second_lag, 2, relay_second)

        @pl.when(t == 1)
        def _():
            for k in range(3):
                weight_along_y(k).wait_recv()
            weight_along_x(0).start()

        when(t == 0, lambda: loads[3].wait())

        @pl.when(t == CHUNKS)
        def _():
            weight_along_x(0).wait_recv()
            weight_along_x(1).start()
            weight_along_x(2).start()

        when(t == 3, lambda: queries(0))
        when(t == half_step, lambda: sibling_arrivals(0, HALF_READY))
        when((t >= half_step) & (t < half_step + half_units), lambda: attend(t - half_step, 0, 0))
        when(t == 9, lambda: queries(1))
        when((t == CHUNKS + 1) & jnp.logical_not(late), lambda: attend(0, 1, 0))
        return carry

    lax.fori_loop(0, CHUNKS + 3, step, 0)
    sibling_arrivals(HALF_READY, CHUNKS)
    loads[4].wait()

    def unit_exchange(u):
        return remote(att.at[head, u], att.at[head, u], att_send.at[u], att_recv.at[u], partner)

    def unit_arrival(u):
        return remote(att.at[head, u], att.at[other, u], att_send.at[u], att_recv.at[u], partner)

    def project(tile, which, groups, fresh):
        rows = slice(tile * TILE, (tile + 1) * TILE)

        def columns_of(j, carry):
            columns = aligned(j * 896, 896)
            product = None
            for group in groups:
                term = jnp.dot(
                    att[which, 2 * tile + group], wob[aligned(which * 1024 + group * 512, 512), columns],
                    preferred_element_type=F32,
                )
                product = term if product is None else product + term
            if fresh:
                branch[rows, columns] = product
            else:
                branch[rows, columns] += product
            return carry

        lax.fori_loop(0, HALF // 896, columns_of, 0)

    for tile in range(2):
        def second_phase(group, carry):
            u = 2 * tile + group
            if tile == 0:
                when(late & (group == 1), lambda: attend(1, 0, 0))
            attend(group, tile, 1)
            denominator = jnp.sum(den[u], axis=-1, keepdims=True)
            attended = (acc[u] / denominator).astype(BF16)
            att[head, u] = jnp.concatenate([attended[:TILE], attended[TILE:]], axis=1)
            unit_exchange(u).start()
            return carry

        lax.fori_loop(0, 2, second_phase, 0)
        if tile == 0:
            when(late, lambda: attend(0, 1, 0))
            attend(1, 1, 0)
        else:
            project(0, head, (0, 1), True)
            for hop in (1, 2):
                weight_along_x(hop).wait_recv()
            weight_sibling().start()
            project(1, head, (0, 1), True)

    diagonal = lax.broadcasted_iota(jnp.int32, (128, 128), 0) == lax.broadcasted_iota(jnp.int32, (128, 128), 1)

    def sums_copy(tile):
        return remote(sums.at[0, tile], sums.at[1, tile], sum_send.at[tile], sum_recv.at[tile], partner)

    def send_sums(tile):
        share = branch[aligned(tile * TILE, TILE)]
        totals = jnp.sum(share * share, axis=-1, keepdims=True)
        for block in range(2):
            spread = jnp.where(diagonal, totals[block * 128 : (block + 1) * 128], 0.0)
            sums[0, tile, block * 8 : (block + 1) * 8] = jnp.broadcast_to(jnp.sum(spread, axis=0, keepdims=True), (8, 128))
        sums_copy(tile).start()

    def output_copy(tile):
        rows = aligned(tile * TILE, TILE)
        return pltpu.make_async_copy(obuf.at[rows], out.at[rows], out_sem.at[tile])

    def finish(tile):
        sums_copy(tile).wait_recv()
        for block in range(2):
            rows = aligned(tile * TILE + block * 128, 128)
            both = sums[0, tile, block * 8 : block * 8 + 1] + sums[1, tile, block * 8 : block * 8 + 1]
            squares = jnp.sum(jnp.where(diagonal, both, 0.0), axis=1, keepdims=True)
            inverse = lax.rsqrt(squares / D + norm_epsilon)
            obuf[rows] = (xbuf[head, rows].astype(F32) + post[...][None, :] * branch[rows] * inverse).astype(BF16)
        output_copy(tile).start()

    def drain(c):
        token_copy(c).wait_send()
        when(far_direct(c), lambda: far(c).wait_send())
        when(far_by_transit(c), lambda: far_transit(c).wait_send())
        when(onward_here(c), lambda: onward(c).wait_send())
        if c[1] < PART:
            when(goes_across, lambda: across(c).wait_send())
        when(up_own | up_relay, lambda: up(c).wait_send())
        when(down_valid(c), lambda: down(c).wait_send())
        when(second_up_valid(c), lambda: second_up(c).wait_send())
        when(second_down_valid(c), lambda: second_down(c).wait_send())
        for slot in (0, 2, 4, 6, 8):
            sends = (slot <= s) & ((core == 0) if slot == 0 else (core == 1) if slot == 8 else (core >= 0))
            when(sends, lambda: to_sibling(c, slot).wait_send())

    weight_sibling().wait_recv()
    unit_arrival(0).wait_recv()
    unit_arrival(1).wait_recv()
    project(0, other, (0, 1), False)
    send_sums(0)
    unit_arrival(2).wait_recv()
    project(1, other, (0,), False)
    each_chunk(0, CHUNKS, drain)
    weight_slice().wait_send()
    for k in range(3):
        weight_along_y(k).wait_send()
        weight_along_x(k).wait_send()
    weight_sibling().wait_send()
    unit_arrival(3).wait_recv()
    project(1, other, (1,), False)
    send_sums(1)
    finish(0)
    finish(1)

    for u in range(UNITS):
        unit_exchange(u).wait_send()
    for tile in range(2):
        sums_copy(tile).wait_send()
        output_copy(tile).wait()


def local(tokens, pre_gain, query_weight, key_weight, value_weight, out_weight, post_gain):
    turns, frequency = rope_rows()
    vmem = pl.BlockSpec(memory_space=pltpu.VMEM)
    hbm = pl.BlockSpec(memory_space=pl.ANY)
    dma = pltpu.SemaphoreType.DMA
    return pl.pallas_call(
        layer_kernel,
        out_shape=jax.ShapeDtypeStruct((ROWS, HALF), BF16),
        in_specs=[hbm, vmem, hbm, hbm, hbm, hbm, vmem, vmem, vmem],
        out_specs=hbm,
        scratch_shapes=[
            pltpu.VMEM((2, ROWS, HALF), BF16),
            pltpu.VMEM((ROWS, D), BF16),
            pltpu.VMEM((D, 4 * HD), BF16),
            pltpu.VMEM((D, 2 * HD), BF16),
            pltpu.VMEM((D, 2 * HD), BF16),
            pltpu.VMEM((2048, HALF), BF16),
            pltpu.VMEM((4, ROWS, HD), BF16),
            pltpu.VMEM((SLOTS * ROWS, 4 * HD), BF16),
            pltpu.VMEM((UNITS, 2 * TILE, HD), F32),
            pltpu.VMEM((UNITS, 2 * TILE, 128), F32),
            pltpu.VMEM((2, UNITS, TILE, 2 * HD), BF16),
            pltpu.VMEM((ROWS, HALF), F32),
            pltpu.VMEM((3, PART, 4 * HD), BF16),
            pltpu.VMEM((2, 2, 16, 128), F32),
            pltpu.VMEM((ROWS, HALF), BF16),
            pltpu.VMEM((ROWS, HD // 2), F32),
            pltpu.VMEM((ROWS, HD // 2), F32),
            dma((5,)),
            dma((CHUNKS,)),
            dma((CHUNKS,)),
            dma((5, CHUNKS)),
            dma((4, CHUNKS)),
            dma((4, CHUNKS)),
            dma((4, CHUNKS)),
            dma((CHUNKS,)),
            dma((3,)),
            dma((3,)),
            dma((2,)),
            dma((8,)),
            dma((8,)),
            dma((UNITS,)),
            dma((UNITS,)),
            dma((2,)),
            dma((2,)),
            dma((2,)),
        ],
        compiler_params=pltpu.CompilerParams(
            collective_id=0, has_side_effects=True, vmem_limit_bytes=63 * 1024 * 1024
        ),
        name="layer",
    )(
        tokens, pre_gain, query_weight, key_weight, value_weight, out_weight,
        post_gain, turns, frequency,
    )


def solution(mesh):
    placed = (
        P("seq", "head"),
        P(),
        P(None, "head"),
        P(None, "head"),
        P(None, "head"),
        P("head", None),
        P("head"),
    )
    return jax.shard_map(
        local, mesh=mesh, in_specs=placed, out_specs=P("seq", "head"), check_vma=False
    )
```

```python
import math

import jax
import jax.numpy as jnp
import numpy as np
from jax import lax
from jax.experimental import pallas as pl
from jax.experimental.pallas import tpu as pltpu
from jax.sharding import PartitionSpec as P

D = 3584
HALF = 1792
HD = 256
ROWS = 512
PART = 64
LONG = 7
CHUNKS = 9
HALF_READY = 4
SLOTS = 9
TILE = 256
UNITS = 4
MESH = pl.DeviceIdType.MESH
F32 = jnp.float32
BF16 = jnp.bfloat16
softcap_limit = 50.0
rope_base = 10000.0
norm_epsilon = 1e-06
EXP_SCALE = softcap_limit * math.log2(math.e)
SCORE_SCALE = HD ** (-0.5) / softcap_limit


def rope_rows():
    frequency = rope_base ** (-2.0 * np.arange(HD // 2) / HD)
    angles = np.arange(ROWS)[:, None] * frequency[None, :]
    table = np.stack([np.cos(angles), np.sin(angles)])
    return table.astype(np.float32), np.broadcast_to(frequency, (8, HD // 2)).astype(np.float32)


def aligned(start, size, step=None):
    return pl.ds(pl.multiple_of(start, step or size), size)


def chunk_rows(chunk, offset=0):
    index, size = chunk
    start = index * PART if size == PART else LONG * PART + (index - LONG) * size
    return aligned(offset + start, size)


def slot_rows(slot, chunk):
    return chunk_rows(chunk, (SLOTS - 1 - slot) * ROWS)


def each_chunk(first, last, action):
    def over(low, high, size):
        def one(i, carry):
            action((i, size))
            return carry

        lax.fori_loop(low, high, one, 0)

    over(first, jnp.minimum(last, LONG), PART)
    over(jnp.maximum(first, LONG), last, PART // 2)


def when(condition, action):
    pl.when(condition)(action)


def layer_kernel(
    tok, gain, wq, wk, wv, wo, post, turns, frequency, out,
    xbuf, xn, wqb, wkb, wvb, wob, q, kv, acc, den, att, branch, transit, sums, obuf, cosine, sine,
    load_sem, z_send, z_recv, send, recv, pair_send, pair_recv,
    transit_send, transit_recv, onward_send, across_send, w_send, w_recv, att_send, att_recv, sum_send, sum_recv, out_sem,
):
    s = lax.axis_index("seq")
    head = lax.axis_index("head")
    core = lax.rem(s, 2)
    chip = lax.div(s, 2)
    y = lax.rem(chip, 4)
    x = lax.rem(lax.div(chip, 4), 4)
    z = lax.div(chip, 16)
    other = 1 - head
    seq_up = s + jnp.where(y < 3, 2, -6)
    seq_down = s + jnp.where(y > 0, -2, 6)
    sibling = s + 1 - 2 * core
    has_next = chip < 28
    has_prev = chip >= 4
    crosses = (z == 0) & (x == 3)
    ring_y = [s + 2 * (lax.rem(y + k, 4) - y) for k in (1, 2, 3)]
    ring_x = [s + 8 * (lax.rem(x + k, 4) - x) for k in (1, 2, 3)]

    def at_seq(target):
        return (target, head)

    partner = (s, other)
    weight_partner = (s + 32 - 64 * z, other)

    def remote(source, target, send_sem, recv_sem, device):
        return pltpu.make_async_remote_copy(
            src_ref=source, dst_ref=target, send_sem=send_sem, recv_sem=recv_sem,
            device_id=device, device_id_type=MESH,
        )

    own_columns = aligned(head * HALF, HALF, 128)
    other_columns = aligned(other * HALF, HALF, 128)
    loads = [
        pltpu.make_async_copy(tok, xbuf.at[head], load_sem.at[0]),
        pltpu.make_async_copy(wv, wvb, load_sem.at[1]),
        pltpu.make_async_copy(wk, wkb, load_sem.at[2]),
        pltpu.make_async_copy(wq, wqb, load_sem.at[3]),
        pltpu.make_async_copy(wo.at[:, own_columns], wob.at[aligned(head * 1024, 1024)], load_sem.at[4]),
    ]
    for load in loads:
        load.start()

    barrier = pltpu.get_barrier_semaphore()

    def greet(device):
        pl.semaphore_signal(barrier, inc=1, device_id=device, device_id_type=MESH)

    greet(partner)
    greet(weight_partner)
    greet(at_seq(sibling))
    for target in ring_y + ring_x:
        greet(at_seq(target))

    @pl.when(z == 1)
    def _():
        greet(at_seq((12 + y) * 2 + core))

    @pl.when(crosses)
    def _():
        for column in range(4):
            greet(at_seq((16 + 4 * column + y) * 2 + core))

    @pl.when(crosses & (y >= 1))
    def _():
        greet(at_seq(jnp.where(y == 1, 16, 14 + y) * 2 + core))

    @pl.when((z == 1) & (x == 0) & (y < 2))
    def _():
        greet(at_seq((14 + y) * 2 + core))

    @pl.when((z == 1) & (x == 0) & (y == 0))
    def _():
        greet(at_seq(13 * 2 + core))

    pairs_across = jnp.where(crosses, jnp.minimum(y, 1), jnp.where((z == 1) & (x == 0), jnp.maximum(2 - y, 0), 0))
    pl.semaphore_wait(barrier, 9 + z + 4 * crosses.astype(jnp.int32) + pairs_across)

    slice_index = (core * 4 + x) * 4 + y
    mine = head * 1024
    theirs = other * 1024

    def weight_slice():
        return remote(
            wo.at[aligned(slice_index * 32, 32), other_columns], wob.at[aligned(mine + slice_index * 32, 32)],
            w_send.at[0], w_recv.at[0], weight_partner,
        )

    def weight_along_y(k):
        rows = aligned(theirs + slice_index * 32, 32)
        return remote(wob.at[rows], wob.at[rows], w_send.at[1 + k], w_recv.at[1 + k], at_seq(ring_y[k]))

    def weight_along_x(hop):
        column = lax.rem(x + 1, 4) if hop == 1 else x
        rows = aligned(theirs + (core * 4 + column) * 128, 128)
        return remote(wob.at[rows], wob.at[rows], w_send.at[4 + hop], w_recv.at[4 + hop], at_seq(ring_x[0 if hop == 2 else 2]))

    def weight_sibling():
        rows = aligned(theirs + core * 512, 512)
        return remote(wob.at[rows], wob.at[rows], w_send.at[7], w_recv.at[7], at_seq(sibling))

    def token_copy(c):
        rows = chunk_rows(c)
        return remote(tok.at[rows], xbuf.at[head, rows], z_send.at[c[0]], z_recv.at[c[0]], partner)

    def token_arrival(c):
        rows = chunk_rows(c)
        return remote(tok.at[rows], xbuf.at[other, rows], z_send.at[c[0]], z_recv.at[c[0]], partner)

    def flow(index, c, source, slot, target):
        return remote(
            kv.at[slot_rows(source, c)], kv.at[slot_rows(slot, c)], send.at[index, c[0]], recv.at[index, c[0]],
            at_seq(target),
        )

    def far(c):
        return flow(0, c, 0, 8, s + 8)

    def transit_slot(c):
        return transit.at[lax.div(c[0], 3), pl.ds(0, c[1])]

    def far_transit(c):
        column = column_of(c)
        return remote(
            kv.at[slot_rows(0, c)], transit_slot(c), transit_send.at[c[0]], transit_recv.at[lax.div(c[0], 3)],
            at_seq((16 + 4 * column + y) * 2 + core),
        )

    def onward(c):
        return remote(
            transit_slot(c), kv.at[slot_rows(8, c)], onward_send.at[lax.div(c[0], 3)], recv.at[0, c[0]], at_seq(s - 8 * x)
        )

    def column_of(c):
        return jnp.where(c[0] < LONG - 1, lax.rem(c[0], 3), jnp.where(c[0] == LONG - 1, 3, 0))

    def in_own_column(c):
        return column_of(c) == 0

    def far_direct(c):
        return has_next & ((z == 1) | (x < 3) | in_own_column(c))

    def far_by_transit(c):
        return crosses & jnp.logical_not(in_own_column(c))

    def onward_here(c):
        return (z == 1) & (x > 0) & (column_of(c) == x)

    def across(c):
        return remote(
            kv.at[slot_rows(0, c)], kv.at[slot_rows(jnp.where(y == 1, 6, 4), c)], across_send.at[c[0] - LONG],
            recv.at[jnp.where(y == 1, 2, 3), c[0]], at_seq(across_target),
        )

    def up(c):
        return flow(1, c, jnp.where(y < 3, 0, 8), 2, seq_up)

    def down(c):
        return flow(2, c, jnp.where(y == 0, 0, 8), 6, seq_down)

    def second_up(c):
        return flow(3, c, 2, 4, seq_up)

    def second_down(c):
        return remote(
            kv.at[slot_rows(6, c)], kv.at[slot_rows(4, c)], send.at[4, c[0]], recv.at[3, c[0]], at_seq(seq_down)
        )

    def to_sibling(c, slot):
        target = slot + 1 - 2 * core
        lane = lax.div(target - 1, 2)
        return remote(
            kv.at[slot_rows(slot, c)], kv.at[slot_rows(target, c)], pair_send.at[lane, c[0]], pair_recv.at[lane, c[0]],
            at_seq(sibling),
        )

    up_own = y < 3
    up_relay = (y == 3) & has_prev
    down_own = y == 0
    crossed = (z == 1) & (x == 0)
    goes_across = crosses & (y >= 1)
    across_target = jnp.where(y == 1, 16, 14 + y) * 2 + core

    def down_valid(c):
        relays = (y > 0) & has_prev
        return down_own | (relays if c[1] == PART else relays & jnp.logical_not(crossed & (y == 1)))

    def second_up_valid(c):
        valid = (y < 3) & (chip >= 1)
        return valid if c[1] == PART else valid & jnp.logical_not(crossed & (y == 0))

    def second_down_valid(c):
        valid = (y == 1) & has_prev
        return valid if c[1] == PART else valid & jnp.logical_not(crossed)


    weight_slice().start()
    each_chunk(0, CHUNKS, lambda c: token_copy(c).start())
    base = jnp.sum(jnp.where(lax.broadcasted_iota(jnp.int32, (8, HD // 2), 0) == 0, frequency[...], 0.0), axis=0, keepdims=True)
    base = base * (s * ROWS).astype(F32)
    base_cos = jnp.cos(base)
    base_sin = jnp.sin(base)
    cosine[...] = base_cos * turns[0] - base_sin * turns[1]
    sine[...] = base_sin * turns[0] + base_cos * turns[1]
    for load in loads[:3]:
        load.wait()
    weight_slice().wait_recv()
    for k in range(3):
        weight_along_y(k).start()

    def roped(values, rows):
        cos = cosine[rows]
        sin = sine[rows]
        leading = values[:, : HD // 2]
        trailing = values[:, HD // 2 :]
        return jnp.concatenate([leading * cos - trailing * sin, trailing * cos + leading * sin], axis=1).astype(BF16)

    def own(c):
        token_arrival(c).wait_recv()
        rows = chunk_rows(c)
        first = xbuf[0, rows].astype(F32)
        second = xbuf[1, rows].astype(F32)
        squares = jnp.sum(first * first, axis=-1, keepdims=True) + jnp.sum(second * second, axis=-1, keepdims=True)
        scale = lax.rsqrt(squares / D + norm_epsilon)
        xn[rows, :HALF] = (first * scale * gain[:HALF][None, :]).astype(BF16)
        xn[rows, HALF:] = (second * scale * gain[HALF:][None, :]).astype(BF16)

        def value(j, carry):
            product = jnp.dot(xn[rows], wvb[:, aligned(j * HD, HD)], preferred_element_type=F32)
            kv[slot_rows(0, c), aligned(2 * HD + j * HD, HD)] = product.astype(BF16)
            return carry

        def key(j, carry):
            columns = aligned(j * HD, HD)
            product = jnp.dot(xn[rows], wkb[:, columns], preferred_element_type=F32)
            kv[slot_rows(0, c), columns] = roped(product, rows)
            return carry

        lax.fori_loop(0, 2, value, 0)
        lax.fori_loop(0, 2, key, 0)
        when(far_direct(c), lambda: far(c).start())
        when(far_by_transit(c), lambda: far_transit(c).start())
        if c[1] < PART:
            when(goes_across, lambda: across(c).start())
        when(up_own, lambda: up(c).start())
        when(down_own, lambda: down(c).start())
        when(core == 0, lambda: to_sibling(c, 0).start())

    def queries(tile):
        rows = aligned(tile * TILE, TILE)

        def query(j, carry):
            product = jnp.dot(xn[rows], wqb[:, aligned(j * HD, HD)], preferred_element_type=F32)
            q[j, rows] = roped(product, rows)
            return carry

        lax.fori_loop(0, 4, query, 0)

    def relay_onward(c):
        @pl.when(onward_here(c))
        def _():
            far_transit(c).wait_recv()
            onward(c).start()

    def relay_far(c):
        @pl.when(has_prev)
        def _():
            far(c).wait_recv()
            when(up_relay, lambda: up(c).start())
            when(down_valid(c) & (y > 0), lambda: down(c).start())
            when(core == 1, lambda: to_sibling(c, 8).start())

    def relay_up(c):
        @pl.when(chip >= 1)
        def _():
            up(c).wait_recv()
            when(second_up_valid(c), lambda: second_up(c).start())
            to_sibling(c, 2).start()

    def relay_down(c):
        @pl.when(chip >= 3)
        def _():
            down(c).wait_recv()
            when(second_down_valid(c), lambda: second_down(c).start())
            to_sibling(c, 6).start()

    def relay_second(c):
        @pl.when(chip >= 2)
        def _():
            second_up(c).wait_recv()
            to_sibling(c, 4).start()

    def sibling_arrivals(first, last):
        def arrivals(c):
            for lane in range(4):
                @pl.when(s >= 2 * lane + 1)
                def _():
                    rows = slot_rows(2 * lane + 1, c)
                    remote(
                        kv.at[rows], kv.at[rows], pair_send.at[lane, c[0]], pair_recv.at[lane, c[0]], at_seq(sibling)
                    ).wait_recv()

        each_chunk(first, last, arrivals)

    query_row = lax.rem(lax.broadcasted_iota(jnp.int32, (2 * TILE, TILE), 0), TILE)
    key_row = lax.broadcasted_iota(jnp.int32, (2 * TILE, TILE), 1)

    def attend(group, tile, phase):
        u = 2 * tile + group
        key_columns = aligned(group * HD, HD)
        value_columns = aligned(2 * HD + group * HD, HD)
        query = q[pl.ds(2 * group, 2), tile * TILE : (tile + 1) * TILE].reshape(2 * TILE, HD)

        def block(slot, mask):
            rows = aligned((SLOTS - 1 - slot) * ROWS + phase * TILE, TILE)
            scores = lax.dot_general(
                query, kv[rows, key_columns], (((1,), (1,)), ((), ())), preferred_element_type=F32
            )
            weights = jnp.exp2(EXP_SCALE * jnp.tanh(scores * SCORE_SCALE))
            if mask is not None:
                weights = jnp.where(mask, weights, 0.0)
            product = jnp.dot(weights.astype(BF16), kv[rows, value_columns], preferred_element_type=F32)
            return weights[:, :128] + weights[:, 128:], product

        def add(parts, fresh):
            partial, product = parts[0]
            for more_partial, more_product in parts[1:]:
                partial = partial + more_partial
                product = product + more_product
            if fresh:
                den[u] = partial
                acc[u] = product
            else:
                den[u] += partial
                acc[u] += product

        def causal():
            return block(0, (key_row <= query_row) if tile == phase else None)

        def edge():
            return block(8, (key_row > query_row) if tile == phase else None)

        has_causal = phase <= tile
        has_edge = phase >= tile

        @pl.when(s >= 8)
        def _():
            parts = [block(slot, None) for slot in range(1, 8)]
            if has_causal:
                parts.insert(0, causal())
            if has_edge:
                parts.append(edge())
            add(parts, phase == 0)

        @pl.when(s < 8)
        def _():
            if phase == 0:
                add([causal()], True)
            elif has_causal:
                add([causal()], False)

            def single(j, carry):
                add([block(1 + j, None)], False)
                return carry

            def triple(j, carry):
                add([block(1 + 3 * j + k, None) for k in range(3)], False)
                return carry

            triples = lax.div(s, 3)
            lax.fori_loop(0, triples, triple, 0)
            lax.fori_loop(3 * triples, jnp.minimum(7, s), single, 0)

    late = has_prev
    far_lag = jnp.where(crossed, 2, 1)
    near_lag = jnp.where(far_lag == 1, 2, far_lag + 1)
    up_lag = jnp.where(y == 0, near_lag, 2)
    down_lag = jnp.where(y == 3, 2, near_lag)
    second_lag = jnp.where(y < 2, near_lag + 2, 4)
    half_step = jnp.where(late, CHUNKS + 1, jnp.maximum(jnp.maximum(up_lag, down_lag), second_lag) + HALF_READY - 1)
    half_units = jnp.where(late, 1, 2)

    def relayed(t, lag, hops):
        return jnp.where(
            t >= CHUNKS + hops // 2, jnp.minimum(t - hops, CHUNKS), jnp.clip(t + 1 - lag, 0, CHUNKS)
        )

    def relay(t, lag, hops, action):
        each_chunk(relayed(t - 1, lag, hops), relayed(t, lag, hops), action)

    def step(t, carry):
        each_chunk(t, jnp.minimum(t + 1, CHUNKS), own)
        each_chunk(jnp.maximum(t - 2, 0), jnp.clip(t - 1, 0, CHUNKS), relay_onward)
        relay(t, far_lag, 0, relay_far)
        relay(t, up_lag, 1, relay_up)
        relay(t, down_lag, 1, relay_down)
        relay(t, second_lag, 2, relay_second)

        @pl.when(t == 1)
        def _():
            for k in range(3):
                weight_along_y(k).wait_recv()
            weight_along_x(0).start()

        when(t == 0, lambda: loads[3].wait())

        @pl.when(t == CHUNKS)
        def _():
            weight_along_x(0).wait_recv()
            weight_along_x(1).start()
            weight_along_x(2).start()

        when(t == 3, lambda: queries(0))
        when(t == half_step, lambda: sibling_arrivals(0, HALF_READY))
        when((t >= half_step) & (t < half_step + half_units), lambda: attend(t - half_step, 0, 0))
        when(t == 9, lambda: queries(1))
        when((t == CHUNKS + 1) & jnp.logical_not(late), lambda: attend(0, 1, 0))
        return carry

    lax.fori_loop(0, CHUNKS + 3, step, 0)
    sibling_arrivals(HALF_READY, CHUNKS)
    loads[4].wait()

    def unit_exchange(u):
        return remote(att.at[head, u], att.at[head, u], att_send.at[u], att_recv.at[u], partner)

    def unit_arrival(u):
        return remote(att.at[head, u], att.at[other, u], att_send.at[u], att_recv.at[u], partner)

    def project(tile, which, groups, fresh):
        rows = slice(tile * TILE, (tile + 1) * TILE)

        def columns_of(j, carry):
            columns = aligned(j * 896, 896)
            product = None
            for group in groups:
                term = jnp.dot(
                    att[which, 2 * tile + group], wob[aligned(which * 1024 + group * 512, 512), columns],
                    preferred_element_type=F32,
                )
                product = term if product is None else product + term
            if fresh:
                branch[rows, columns] = product
            else:
                branch[rows, columns] += product
            return carry

        lax.fori_loop(0, HALF // 896, columns_of, 0)

    for tile in range(2):
        def second_phase(group, carry):
            u = 2 * tile + group
            if tile == 0:
                when(late & (group == 1), lambda: attend(1, 0, 0))
            attend(group, tile, 1)
            denominator = jnp.sum(den[u], axis=-1, keepdims=True)
            attended = (acc[u] / denominator).astype(BF16)
            att[head, u] = jnp.concatenate([attended[:TILE], attended[TILE:]], axis=1)
            unit_exchange(u).start()
            return carry

        lax.fori_loop(0, 2, second_phase, 0)
        if tile == 0:
            when(late, lambda: attend(0, 1, 0))
            attend(1, 1, 0)
        else:
            project(0, head, (0, 1), True)
            for hop in (1, 2):
                weight_along_x(hop).wait_recv()
            weight_sibling().start()
            project(1, head, (0, 1), True)

    diagonal = lax.broadcasted_iota(jnp.int32, (128, 128), 0) == lax.broadcasted_iota(jnp.int32, (128, 128), 1)

    def sums_copy(tile):
        return remote(sums.at[0, tile], sums.at[1, tile], sum_send.at[tile], sum_recv.at[tile], partner)

    def send_sums(tile):
        share = branch[aligned(tile * TILE, TILE)]
        totals = jnp.sum(share * share, axis=-1, keepdims=True)
        for block in range(2):
            spread = jnp.where(diagonal, totals[block * 128 : (block + 1) * 128], 0.0)
            sums[0, tile, block * 8 : (block + 1) * 8] = jnp.broadcast_to(jnp.sum(spread, axis=0, keepdims=True), (8, 128))
        sums_copy(tile).start()

    def output_copy(tile):
        rows = aligned(tile * TILE, TILE)
        return pltpu.make_async_copy(obuf.at[rows], out.at[rows], out_sem.at[tile])

    def finish(tile):
        sums_copy(tile).wait_recv()
        for block in range(2):
            rows = aligned(tile * TILE + block * 128, 128)
            both = sums[0, tile, block * 8 : block * 8 + 1] + sums[1, tile, block * 8 : block * 8 + 1]
            squares = jnp.sum(jnp.where(diagonal, both, 0.0), axis=1, keepdims=True)
            inverse = lax.rsqrt(squares / D + norm_epsilon)
            obuf[rows] = (xbuf[head, rows].astype(F32) + post[...][None, :] * branch[rows] * inverse).astype(BF16)
        output_copy(tile).start()

    def drain(c):
        token_copy(c).wait_send()
        when(far_direct(c), lambda: far(c).wait_send())
        when(far_by_transit(c), lambda: far_transit(c).wait_send())
        when(onward_here(c), lambda: onward(c).wait_send())
        if c[1] < PART:
            when(goes_across, lambda: across(c).wait_send())
        when(up_own | up_relay, lambda: up(c).wait_send())
        when(down_valid(c), lambda: down(c).wait_send())
        when(second_up_valid(c), lambda: second_up(c).wait_send())
        when(second_down_valid(c), lambda: second_down(c).wait_send())
        for slot in (0, 2, 4, 6, 8):
            sends = (slot <= s) & ((core == 0) if slot == 0 else (core == 1) if slot == 8 else (core >= 0))
            when(sends, lambda: to_sibling(c, slot).wait_send())

    weight_sibling().wait_recv()
    unit_arrival(0).wait_recv()
    unit_arrival(1).wait_recv()
    project(0, other, (0, 1), False)
    send_sums(0)
    unit_arrival(2).wait_recv()
    project(1, other, (0,), False)
    each_chunk(0, CHUNKS, drain)
    weight_slice().wait_send()
    for k in range(3):
        weight_along_y(k).wait_send()
        weight_along_x(k).wait_send()
    weight_sibling().wait_send()
    unit_arrival(3).wait_recv()
    project(1, other, (1,), False)
    send_sums(1)
    finish(0)
    finish(1)

    for u in range(UNITS):
        unit_exchange(u).wait_send()
    for tile in range(2):
        sums_copy(tile).wait_send()
        output_copy(tile).wait()


def local(tokens, pre_gain, query_weight, key_weight, value_weight, out_weight, post_gain):
    turns, frequency = rope_rows()
    vmem = pl.BlockSpec(memory_space=pltpu.VMEM)
    hbm = pl.BlockSpec(memory_space=pl.ANY)
    dma = pltpu.SemaphoreType.DMA
    return pl.pallas_call(
        layer_kernel,
        out_shape=jax.ShapeDtypeStruct((ROWS, HALF), BF16),
        in_specs=[hbm, vmem, hbm, hbm, hbm, hbm, vmem, vmem, vmem],
        out_specs=hbm,
        scratch_shapes=[
            pltpu.VMEM((2, ROWS, HALF), BF16),
            pltpu.VMEM((ROWS, D), BF16),
            pltpu.VMEM((D, 4 * HD), BF16),
            pltpu.VMEM((D, 2 * HD), BF16),
            pltpu.VMEM((D, 2 * HD), BF16),
            pltpu.VMEM((2048, HALF), BF16),
            pltpu.VMEM((4, ROWS, HD), BF16),
            pltpu.VMEM((SLOTS * ROWS, 4 * HD), BF16),
            pltpu.VMEM((UNITS, 2 * TILE, HD), F32),
            pltpu.VMEM((UNITS, 2 * TILE, 128), F32),
            pltpu.VMEM((2, UNITS, TILE, 2 * HD), BF16),
            pltpu.VMEM((ROWS, HALF), F32),
            pltpu.VMEM((3, PART, 4 * HD), BF16),
            pltpu.VMEM((2, 2, 16, 128), F32),
            pltpu.VMEM((ROWS, HALF), BF16),
            pltpu.VMEM((ROWS, HD // 2), F32),
            pltpu.VMEM((ROWS, HD // 2), F32),
            dma((5,)),
            dma((CHUNKS,)),
            dma((CHUNKS,)),
            dma((5, CHUNKS)),
            dma((4, CHUNKS)),
            dma((4, CHUNKS)),
            dma((4, CHUNKS)),
            dma((CHUNKS,)),
            dma((3,)),
            dma((3,)),
            dma((2,)),
            dma((8,)),
            dma((8,)),
            dma((UNITS,)),
            dma((UNITS,)),
            dma((2,)),
            dma((2,)),
            dma((2,)),
        ],
        compiler_params=pltpu.CompilerParams(
            collective_id=0, has_side_effects=True, vmem_limit_bytes=63 * 1024 * 1024
        ),
        name="layer",
    )(
        tokens, pre_gain, query_weight, key_weight, value_weight, out_weight,
        post_gain, turns, frequency,
    )


def solution(mesh):
    placed = (
        P("seq", "head"),
        P(),
        P(None, "head"),
        P(None, "head"),
        P(None, "head"),
        P("head", None),
        P("head"),
    )
    return jax.shard_map(
        local, mesh=mesh, in_specs=placed, out_specs=P("seq", "head"), check_vma=False
    )
```
